128 devices in a mesh: pair: 2 (over x_hi), seq: 32 (over z, y, core), head: 2 (over x_lo).
Axes of the slice: x: 4 (x_hi: 2, x_lo: 2; x = x_hi * 2 + x_lo), y: 4, z: 4, core: 2. Of those that a mesh axis runs over, the one named last changes fastest.
Arguments:
- queries: bfloat16 [2, 2048, 2, 3584], P('pair', 'seq', None, 'head'), may hold values from -6 to 6
- answer_keys: bfloat16 [2, 2048, 2, 512], P('pair', 'seq', None, 'head'), may hold values from -6 to 6
- answer_values: bfloat16 [2, 2048, 2, 512], P('pair', 'seq', None, 'head'), may hold values from -6 to 6
- prefix_keys: bfloat16 [3072, 512], P(('pair', 'seq'), 'head'), may hold values from -8 to 8
- prefix_values: bfloat16 [3072, 512], P(('pair', 'seq'), 'head'), may hold values from -6 to 6
- grad_out: bfloat16 [2, 2048, 2, 3584], P('pair', 'seq', None, 'head'), may hold values from -6 to 6
- answer_length: int32 [2, 2], P('pair'), may hold values from 512 to 2048
- prefix_limit: int32 [2, 2], P('pair'), may hold values from 1536 to 3072
Outputs:
- attention_out: bfloat16 [2, 2048, 2, 3584], P('pair', 'seq', None, 'head')
- grad_queries: bfloat16 [2, 2048, 2, 3584], P('pair', 'seq', None, 'head')
- grad_answer_keys: bfloat16 [2, 2048, 2, 512], P('pair', 'seq', None, 'head')
- grad_answer_values: bfloat16 [2, 2048, 2, 512], P('pair', 'seq', None, 'head')
- grad_prefix_keys: float32 [3072, 512], P(('pair', 'seq'), 'head')
- grad_prefix_values: float32 [3072, 512], P(('pair', 'seq'), 'head')
The draws below stay inside these ranges and needn't reach their ends.
All inputs are finite; a program needn't handle non-finite values.
Results may differ from the reference program's by a relative error of at most 0.015.
Values may be sent and summed in bfloat16 or wider, within the bound.
A program may use at most 64 MiB of HBM per device.

```python
from functools import partial
import jax
import jax.numpy as jnp
from jax import lax

HEADS = 28
KV_HEADS = 4
HEAD_DIM = 128
BATCH = 2
ANS = 2048
PREFIX = 3072


def draw_queries(key, part):
    shape = (2, ANS, BATCH, HEADS * HEAD_DIM)
    values = jax.random.normal(jax.random.fold_in(key, 11), shape, jnp.float32)
    return jnp.clip(values, -6.0, 6.0).astype(jnp.bfloat16)


def draw_prefix_keys(key, part):
    shape = (PREFIX, KV_HEADS * HEAD_DIM)
    values = jax.random.normal(jax.random.fold_in(key, 13), shape, jnp.float32)
    return jnp.clip(values, -6.0, 6.0).astype(jnp.bfloat16)


def plant(values, rng, smallest, high):
    longest = values.shape.index(max(values.shape))
    spots = []
    for shift in (0, 1):
        where = [jax.random.randint(jax.random.fold_in(rng, axis), (), 0, length) for axis, length in enumerate(values.shape)]
        where[longest] = (where[longest] + shift) % values.shape[longest]
        spots.append(tuple(where))
    return values.at[spots[0]].set(smallest).at[spots[1]].set(high)


def levels(own_key, dims, split, smallest, top_value):
    def one(position, blocks):
        heights = jax.random.uniform(jax.random.fold_in(jax.random.fold_in(own_key, 6), position), (blocks,), jnp.float32, smallest / len(split), top_value / len(split))
        return jnp.repeat(jnp.exp(heights), dims[position] // blocks).reshape((-1,) + (1,) * (len(dims) - position - 1))

    gain = one(*split[0])
    for cut in split[1:]:
        gain = gain * one(*cut)
    return gain


def gaussian(rng, dims, scale, limit, split=(), kind=jnp.bfloat16):
    values = jax.random.normal(rng, dims, jnp.float32) * scale
    if len(split) > 0:
        values = levels(rng, dims, split, -0.22, 0.18) * values
    return jnp.clip(values, min=-limit, max=limit).astype(kind)


def setup_inputs(seed: int = 0) -> dict:
    keys = jax.random.split(jax.random.key(seed), 9)
    return {
        "queries": draw_queries(jax.random.fold_in(keys[8], 71), 0),
        "answer_keys": gaussian(keys[1], (2, ANS, BATCH, KV_HEADS * HEAD_DIM), 1.0, 6.0, ((0, 2), (1, 32), (3, 2))),
        "answer_values": gaussian(keys[2], (2, ANS, BATCH, KV_HEADS * HEAD_DIM), 1.0, 6.0, ((0, 2), (1, 32), (3, 2))),
        "prefix_keys": draw_prefix_keys(jax.random.fold_in(keys[8], 71), 0),
        "prefix_values": gaussian(keys[4], (PREFIX, KV_HEADS * HEAD_DIM), 1.0, 6.0, ((0, 64), (1, 2))),
        "grad_out": gaussian(keys[5], (2, ANS, BATCH, HEADS * HEAD_DIM), 1.0, 6.0, ((0, 2), (1, 32), (3, 2))),
        "answer_length": plant(jax.random.randint(keys[6], (2, BATCH), ANS // 4, ANS + 1), jax.random.fold_in(keys[6], 1), ANS // 4, ANS).astype(jnp.int32),
        "prefix_limit": plant(jax.random.randint(keys[7], (2, BATCH), PREFIX // 2, PREFIX + 1), jax.random.fold_in(keys[7], 1), PREFIX // 2, PREFIX).astype(jnp.int32),
    }


negative_fill = -1e30


def one_head(pair_items, keys_all, values_all, limit_here, length):
    head_queries, head_douts = pair_items
    scaling = HEAD_DIM ** -0.5
    raw_scores = jnp.dot(head_queries, keys_all.T, preferred_element_type=jnp.float32) * scaling
    columns = jnp.arange(PREFIX + ANS, dtype=jnp.int32)[None, :]
    positions = jnp.arange(ANS, dtype=jnp.int32)[:, None]
    allowed = jnp.where(columns < PREFIX, columns < limit_here, columns - PREFIX <= positions)
    masked = jnp.where(allowed, raw_scores, negative_fill)
    top_score = jnp.max(masked, axis=1, keepdims=True)
    exp_total = jnp.sum(jnp.where(allowed, jnp.exp(masked - top_score), 0.0), axis=1, keepdims=True)
    log_total = top_score + jnp.log(exp_total)
    probs = jnp.where(allowed, jnp.exp(raw_scores - log_total), 0.0)
    probs_low = lax.optimization_barrier(probs.astype(jnp.bfloat16))
    live = positions < length
    attended = jnp.where(live, jnp.dot(probs_low, values_all, preferred_element_type=jnp.float32), 0.0)
    douts = jnp.where(live, head_douts, jnp.zeros_like(head_douts))
    grad_probs = jnp.dot(douts, values_all.T, preferred_element_type=jnp.float32)
    delta = jnp.sum(douts.astype(jnp.float32) * attended, axis=1, keepdims=True)
    grad_low = lax.optimization_barrier((probs * (grad_probs - delta)).astype(jnp.bfloat16))
    grad_queries = jnp.dot(grad_low, keys_all, preferred_element_type=jnp.float32) * scaling
    key_terms = jnp.dot(grad_low.T, head_queries, preferred_element_type=jnp.float32) * scaling
    value_terms = jnp.dot(probs_low.T, douts, preferred_element_type=jnp.float32)
    return attended.astype(jnp.bfloat16), grad_queries.astype(jnp.bfloat16), key_terms, value_terms


def reference(queries, answer_keys, answer_values, prefix_keys, prefix_values, grad_out, answer_length, prefix_limit):
    group_size = HEADS // KV_HEADS
    group_width = group_size * HEAD_DIM
    prefix_key_sums = [jnp.zeros((PREFIX, HEAD_DIM), jnp.float32) for head_index in range(KV_HEADS)]
    prefix_value_sums = [jnp.zeros((PREFIX, HEAD_DIM), jnp.float32) for head_index in range(KV_HEADS)]
    out_sides, query_sides, key_sides, value_sides = [], [], [], []
    for side_index in range(2):
        out_items, query_items, key_items, value_items = [], [], [], []
        for answer_index in range(BATCH):
            out_heads, query_heads, key_heads, value_heads = [], [], [], []
            for head_index in range(KV_HEADS):
                key_columns = slice(head_index * HEAD_DIM, (head_index + 1) * HEAD_DIM)
                query_columns = slice(head_index * group_width, (head_index + 1) * group_width)
                keys_all = jnp.concatenate([prefix_keys[:, key_columns], answer_keys[side_index, :, answer_index, key_columns]], axis=0)
                values_all = jnp.concatenate([prefix_values[:, key_columns], answer_values[side_index, :, answer_index, key_columns]], axis=0)
                head_queries = queries[side_index, :, answer_index, query_columns].reshape(ANS, group_size, HEAD_DIM).transpose(1, 0, 2)
                head_douts = grad_out[side_index, :, answer_index, query_columns].reshape(ANS, group_size, HEAD_DIM).transpose(1, 0, 2)
                results = lax.map(partial(one_head, keys_all=keys_all, values_all=values_all, limit_here=prefix_limit[side_index, answer_index], length=answer_length[side_index, answer_index]), (head_queries, head_douts))
                out_heads.append(results[0].transpose(1, 0, 2).reshape(ANS, group_width))
                query_heads.append(results[1].transpose(1, 0, 2).reshape(ANS, group_width))
                key_total = jnp.sum(results[2], axis=0)
                value_total = jnp.sum(results[3], axis=0)
                prefix_key_sums[head_index] = prefix_key_sums[head_index] + key_total[:PREFIX]
                prefix_value_sums[head_index] = prefix_value_sums[head_index] + value_total[:PREFIX]
                key_heads.append(key_total[PREFIX:].astype(jnp.bfloat16))
                value_heads.append(value_total[PREFIX:].astype(jnp.bfloat16))
            out_items.append(jnp.concatenate(out_heads, axis=1))
            query_items.append(jnp.concatenate(query_heads, axis=1))
            key_items.append(jnp.concatenate(key_heads, axis=1))
            value_items.append(jnp.concatenate(value_heads, axis=1))
        out_sides.append(jnp.stack(out_items, axis=1))
        query_sides.append(jnp.stack(query_items, axis=1))
        key_sides.append(jnp.stack(key_items, axis=1))
        value_sides.append(jnp.stack(value_items, axis=1))
    return (jnp.stack(out_sides), jnp.stack(query_sides), jnp.stack(key_sides), jnp.stack(value_sides), jnp.concatenate(prefix_key_sums, axis=1), jnp.concatenate(prefix_value_sums, axis=1))
```

```python
import functools

import jax
import jax.numpy as jnp
from jax import lax
from jax.experimental import pallas as pl
from jax.experimental.pallas import tpu as pltpu
from jax.sharding import PartitionSpec as P

HEAD_DIM = 128
RING = 4
CORES = 2
LOG2E = 1.4426950408889634
NEGATIVE = -1e30
MESH = pl.DeviceIdType.MESH
BF16 = jnp.bfloat16
F32 = jnp.float32


def place():
    s = lax.axis_index("seq")
    return s // (RING * CORES), (s // CORES) % RING, s % CORES


def seq_of(h, p, q, core):
    z, y = (q, p) if h == 0 else (p, q)
    return (z * RING + y) * CORES + core


def grid_at(ref, h, p, q, core):
    if h == 0:
        return ref.at[h, q, p, core]
    return ref.at[h, p, q, core]


def greet():
    z, y, core = place()
    pair = lax.axis_index("pair")
    barrier = pltpu.get_barrier_semaphore()
    peers = []
    for h in range(2):
        p, q = (y, z) if h == 0 else (z, y)
        for d in (1, RING - 1):
            peers.append({"seq": seq_of(h, (p + d) % RING, q, core)})
    peers.append({"seq": seq_of(0, y, z, 1 - core)})
    peers.append({"pair": 1 - pair})
    for peer in peers:
        pl.semaphore_signal(barrier, inc=1, device_id=peer, device_id_type=MESH)
    pl.semaphore_wait(barrier, len(peers))


class Copies:
    def __init__(self, send_sem, recv_sem):
        self.send_sem, self.recv_sem = send_sem, recv_sem
        self.ids = {}
        self.sent = []

    def make(self, key, src, dst, to):
        n = self.ids.setdefault(key, len(self.ids))
        return pltpu.make_async_remote_copy(
            src_ref=src,
            dst_ref=dst,
            send_sem=self.send_sem.at[n],
            recv_sem=self.recv_sem.at[n],
            device_id=to,
            device_id_type=MESH,
        )

    def send(self, key, src, dst, to):
        copy = self.make(key, src, dst, to)
        copy.start()
        self.sent.append(copy)

    def arrived(self, key, dst, to):
        self.make(key, dst, dst, to).wait_recv()

    def finish(self):
        for copy in self.sent:
            copy.wait_send()


GATHER_COPIES = 120
ORDER = (0, 3, 1, 2)


def gather_kernel(ans_rows, pre_rows, ans_ref, pre_ref, out_ref, held, send_sem, recv_sem, local_sem, out_sem):
    z, y, core = place()
    pair = lax.axis_index("pair")
    rows = ans_rows + 2 * pre_rows
    half = rows // 2
    parts = (pl.ds(0, half), pl.ds(half, rows - half))
    pieces = (pl.ds(0, ans_rows), pl.ds(ans_rows, 2 * pre_rows))
    whole = pl.ds(0, rows)
    mine = pl.ds(pl.multiple_of(ans_rows + pair * pre_rows, 16), pre_rows)
    other = pl.ds(pl.multiple_of(ans_rows + (1 - pair) * pre_rows, 16), pre_rows)
    at = ((y, z), (z, y))
    copies = Copies(send_sem, recv_sem)
    stores = []

    def block(h, p, q, part):
        return held.at[h, p, q, part]

    def to(h, dp, dq):
        p, q = at[h]
        return {"seq": seq_of(h, (p + dp) % RING, (q + dq) % RING, core)}

    sibling = {"seq": seq_of(0, y, z, 1 - core)}

    locals_ = []
    for h in range(2):
        p, q = at[h]
        locals_.append(pltpu.make_async_copy(ans_ref.at[h], block(h, p, q, pieces[0]), local_sem.at[2 * h]))
        locals_.append(pltpu.make_async_copy(pre_ref.at[h], block(h, p, q, mine), local_sem.at[2 * h + 1]))
    for copy in locals_:
        copy.start()
    greet()
    for h in range(2):
        p, q = at[h]
        copies.send(("pair", h), pre_ref.at[h], block(h, p, q, mine), {"pair": 1 - pair})

    def forward(h, k, axis, p, q, source, part, direction, key):
        dp, dq = (direction, 0) if axis == 0 else (0, direction)
        ref = block(h, p, q, part)
        copies.send(key, ref, ref, to(h, dp, dq))

    def own_first(piece):
        for h in range(2):
            p, q = at[h]
            for direction in (1, 3):
                forward(h, 0, 0, p, q, None, pieces[piece], direction, ("one", h, direction, piece))
        for h in range(2):
            p, q = at[h]
            for direction in (1, 3):
                forward(h, 0, 1, p, q, None, pieces[piece], direction, ("two", h, 0, direction, piece))

    def spread(h, k):
        p, q = at[h]
        source = (p + ORDER[k]) % RING
        for direction in (1, 3):
            forward(h, k, 1, source, q, None, whole, direction, ("two", h, k, direction, 2))

    def share(h, p, q, key):
        ref = block(h, p, q, whole)
        copies.send(("sib", h, key), ref, grid_at(out_ref, h, p, q, core), sibling)
        n = len(stores)
        store = pltpu.make_async_copy(ref, grid_at(out_ref, h, p, q, core), out_sem.at[n])
        store.start()
        stores.append(store)

    locals_[0].wait()
    locals_[2].wait()
    own_first(0)
    locals_[1].wait()
    locals_[3].wait()
    for h in range(2):
        p, q = at[h]
        copies.arrived(("pair", h), block(h, p, q, other), {"pair": 1 - pair})
    own_first(1)
    for h in range(2):
        p, q = at[h]
        share(h, p, q, (0, 0))

    for direction in (1, 3):
        for h in range(2):
            p, q = at[h]
            source = (p - direction) % RING
            for piece in range(2):
                copies.arrived(("one", h, direction, piece), block(h, source, q, pieces[piece]), to(h, direction, 0))
            forward(h, 0, 0, source, q, None, parts[direction // 2], direction, ("far", h, direction))
            spread(h, ORDER.index((-direction) % RING))
            share(h, source, q, ((-direction) % RING, 0))
    for h in range(2):
        p, q = at[h]
        source = (p + 2) % RING
        for direction in (1, 3):
            copies.arrived(("far", h, direction), block(h, source, q, parts[direction // 2]), to(h, direction, 0))
        spread(h, 3)
        share(h, source, q, (2, 0))
    for k in range(RING):
        for direction in (1, 3):
            for h in range(2):
                p, q = at[h]
                p_source, q_source = (p + ORDER[k]) % RING, (q - direction) % RING
                for piece in (range(2) if k == 0 else (2,)):
                    area = whole if piece == 2 else pieces[piece]
                    copies.arrived(("two", h, k, direction, piece), block(h, p_source, q_source, area), to(h, 0, direction))
                forward(h, k, 1, p_source, q_source, None, parts[direction // 2], direction, ("far2", h, k, direction))
                share(h, p_source, q_source, (ORDER[k], (-direction) % RING))
    for k in range(RING):
        for h in range(2):
            p, q = at[h]
            p_source, q_source = (p + ORDER[k]) % RING, (q + 2) % RING
            for direction in (1, 3):
                copies.arrived(("far2", h, k, direction), block(h, p_source, q_source, parts[direction // 2]), to(h, 0, direction))
            share(h, p_source, q_source, (ORDER[k], 2))
    for h in range(2):
        p, q = at[h]
        for dp in range(RING):
            for dq in range(RING):
                area = grid_at(out_ref, h, (p + dp) % RING, (q + dq) % RING, 1 - core)
                copies.arrived(("sib", h, (dp, dq)), area, sibling)
    for store in stores:
        store.wait()
    copies.finish()


def gather(ans, pre):
    kv, ans_rows, width = ans.shape
    pre_rows = pre.shape[1]
    rows = ans_rows + 2 * pre_rows
    return pl.pallas_call(
        functools.partial(gather_kernel, ans_rows, pre_rows),
        out_shape=jax.ShapeDtypeStruct((kv, RING, RING, CORES, rows, width), ans.dtype),
        in_specs=[pl.BlockSpec(memory_space=pltpu.VMEM)] * 2,
        out_specs=pl.BlockSpec(memory_space=pl.ANY),
        scratch_shapes=[
            pltpu.VMEM((kv, RING, RING, rows, width), ans.dtype),
            pltpu.SemaphoreType.DMA((GATHER_COPIES,)),
            pltpu.SemaphoreType.DMA((GATHER_COPIES,)),
            pltpu.SemaphoreType.DMA((4,)),
            pltpu.SemaphoreType.DMA((32,)),
        ],
        compiler_params=pltpu.CompilerParams(collective_id=0, has_side_effects=True),
        name="gather",
    )(ans, pre)


SCATTER_COPIES = 60


def scatter_kernel(
    ans_rows, pre_rows, terms_ref, ans_out, pre_out, total, beside, far2, near2, far1, near1, swap, send_sem, recv_sem, local_sem
):
    z, y, core = place()
    pair = lax.axis_index("pair")
    rows = ans_rows + 2 * pre_rows
    half = rows // 2
    parts = (pl.ds(0, half), pl.ds(half, rows - half))
    mine = pl.ds(pl.multiple_of(ans_rows + pair * pre_rows, 16), pre_rows)
    other = pl.ds(pl.multiple_of(ans_rows + (1 - pair) * pre_rows, 16), pre_rows)
    at = ((y, z), (z, y))
    copies = Copies(send_sem, recv_sem)
    sibling = {"seq": seq_of(0, y, z, 1 - core)}

    def to(h, dp, dq):
        p, q = at[h]
        return {"seq": seq_of(h, (p + dp) % RING, (q + dq) % RING, core)}

    def column(h, p, c):
        if h == 0:
            return terms_ref.at[h, :, p, c]
        return terms_ref.at[h, p, :, c]

    order = (2, 1, 3, 0)
    loads = {}
    for k in range(RING):
        for h in range(2):
            p = (at[h][0] + order[k]) % RING
            loads[h, k] = pltpu.make_async_copy(column(h, p, core), total.at[h, p], local_sem.at[h * RING + k])
            loads[h, k].start()
    greet()
    for k in range(RING):
        for h in range(2):
            p = (at[h][0] + order[k]) % RING
            copies.send(("sib", h, k), column(h, p, 1 - core), beside.at[h, p], sibling)

    def add(into, other_ref):
        into[...] = (into[...].astype(F32) + other_ref[...].astype(F32)).astype(BF16)

    for k in range(RING):
        for h in range(2):
            p, q = at[h]
            target = (p + order[k]) % RING
            loads[h, k].wait()
            copies.arrived(("sib", h, k), beside.at[h, target], sibling)
            far = (q + 2) % RING
            add(total.at[h, target, far], beside.at[h, target, far])
            for n, direction in enumerate((1, 3)):
                copies.send(
                    ("far2", h, k, n), total.at[h, target, far, parts[n]], far2.at[h, k, n], to(h, 0, direction)
                )
            for d in (1, 3, 0):
                place_q = (q + d) % RING
                add(total.at[h, target, place_q], beside.at[h, target, place_q])
    for k in range(RING):
        for h in range(2):
            p, q = at[h]
            target = (p + order[k]) % RING
            for n, direction in enumerate((1, 3)):
                nearby = (q + direction) % RING
                copies.arrived(("far2", h, k, n), far2.at[h, k, n], to(h, 0, direction))
                add(total.at[h, target, nearby, parts[n]], far2.at[h, k, n])
                copies.send(("near2", h, k, n), total.at[h, target, nearby], near2.at[h, k, n], to(h, 0, direction))

    def settle2(h, k):
        p, q = at[h]
        target = (p + order[k]) % RING
        for n, direction in enumerate((1, 3)):
            copies.arrived(("near2", h, k, n), near2.at[h, k, n], to(h, 0, direction))
        into = total.at[h, target, q]
        into[...] = (
            into[...].astype(F32) + near2[h, k, 0].astype(F32) + near2[h, k, 1].astype(F32)
        ).astype(BF16)

    for h in range(2):
        p, q = at[h]
        settle2(h, 0)
        for n, direction in enumerate((1, 3)):
            copies.send(("far1", h, n), total.at[h, (p + 2) % RING, q, parts[n]], far1.at[h, n], to(h, direction, 0))
    for k in (1, 2):
        n = k - 1
        direction = order[k]
        for h in range(2):
            p, q = at[h]
            settle2(h, k)
            nearby = (p + direction) % RING
            copies.arrived(("far1", h, n), far1.at[h, n], to(h, direction, 0))
            add(total.at[h, nearby, q, parts[n]], far1.at[h, n])
            copies.send(("near1", h, n), total.at[h, nearby, q], near1.at[h, n], to(h, direction, 0))
    for h in range(2):
        settle2(h, 3)
    for h in range(2):
        p, q = at[h]
        for n, direction in enumerate((1, 3)):
            copies.arrived(("near1", h, n), near1.at[h, n], to(h, direction, 0))
        into = total.at[h, p, q]

        def final(area):
            return (
                total[h, p, q, area].astype(F32) + near1[h, 0, area].astype(F32) + near1[h, 1, area].astype(F32)
            )

        swap[0, h] = final(other).astype(BF16)
        copies.send(("swap", h), swap.at[0, h], swap.at[1, h], {"pair": 1 - pair})
        pre_out[h] = final(mine)
        ans_out[h] = final(pl.ds(0, ans_rows)).astype(BF16)
    for h in range(2):
        copies.arrived(("swap", h), swap.at[1, h], {"pair": 1 - pair})
        pre_out[h] = pre_out[h] + swap[1, h].astype(F32)
    copies.finish()


def scatter(terms, ans_rows, pre_rows):
    kv, _, _, _, rows, width = terms.shape
    half = rows // 2
    return pl.pallas_call(
        functools.partial(scatter_kernel, ans_rows, pre_rows),
        out_shape=(
            jax.ShapeDtypeStruct((kv, ans_rows, width), BF16),
            jax.ShapeDtypeStruct((kv, pre_rows, width), F32),
        ),
        in_specs=[pl.BlockSpec(memory_space=pl.ANY)],
        out_specs=(pl.BlockSpec(memory_space=pltpu.VMEM), pl.BlockSpec(memory_space=pltpu.VMEM)),
        scratch_shapes=[
            pltpu.VMEM((kv, RING, RING, rows, width), BF16),
            pltpu.VMEM((kv, RING, RING, rows, width), BF16),
            pltpu.VMEM((kv, RING, 2, half, width), BF16),
            pltpu.VMEM((kv, RING, 2, rows, width), BF16),
            pltpu.VMEM((kv, 2, half, width), BF16),
            pltpu.VMEM((kv, 2, rows, width), BF16),
            pltpu.VMEM((2, kv, pre_rows, width), BF16),
            pltpu.SemaphoreType.DMA((SCATTER_COPIES,)),
            pltpu.SemaphoreType.DMA((SCATTER_COPIES,)),
            pltpu.SemaphoreType.DMA((2 * RING,)),
        ],
        compiler_params=pltpu.CompilerParams(collective_id=1, has_side_effects=True),
        name="scatter",
    )(terms)


def nn(a, b):
    return lax.dot_general(a, b, (((1,), (0,)), ((), ())), preferred_element_type=F32)


def nt(a, b):
    return lax.dot_general(a, b, (((1,), (1,)), ((), ())), preferred_element_type=F32)


ANS_SOURCES = 4
PRE_SOURCES = 8


def attend_kernel(
    ans_here,
    pre_rows,
    group,
    length_ref,
    limit_ref,
    q_ref,
    g_ref,
    kv_ref,
    out_ref,
    dq_ref,
    terms_ref,
    scores,
    weights,
    queries,
    douts,
    queries_t,
    douts_t,
    prefix_terms,
    top,
    row_sum,
    acc_t,
):
    sources = kv_ref.shape[1]
    d = HEAD_DIM
    b = pl.program_id(1)
    s = lax.axis_index("seq")
    scale = d**-0.5
    rows = group * ans_here
    ans_chunk = ANS_SOURCES * ans_here
    pre_chunk = PRE_SOURCES * pre_rows
    per_pair = sources // PRE_SOURCES
    pre_total = 2 * sources * pre_rows
    first_row = s * ans_here
    length = length_ref[0, b]
    limit = limit_ref[0, b]
    ans_at = pl.multiple_of(b * ans_here, ans_here)
    live_here = first_row < length
    n_pre = jnp.where(live_here, (limit + pre_chunk - 1) // pre_chunk, 0)
    n_full = jnp.where(live_here, limit // pre_chunk, 0)
    n_ans = jnp.where(live_here, s // ANS_SOURCES + 1, 0)

    @pl.when(b == 0)
    def _():
        prefix_terms[...] = jnp.zeros_like(prefix_terms)

    terms_ref[0, :, pl.ds(ans_at, ans_here), :] = jnp.zeros((sources, ans_here, 2 * d), BF16)

    def pre_block(i, lanes):
        pair_at, source = i // per_pair, (i % per_pair) * PRE_SOURCES
        row = pl.multiple_of(2 * ans_here + pair_at * pre_rows, 16)
        part = kv_ref[0, pl.ds(source, PRE_SOURCES), pl.ds(row, pre_rows), lanes]
        return part.reshape(pre_chunk, d)

    def ans_block(i, lanes):
        part = kv_ref[0, pl.ds(i * ANS_SOURCES, ANS_SOURCES), pl.ds(ans_at, ans_here), lanes]
        return part.reshape(ans_chunk, d)

    keys_at, values_at = slice(0, d), slice(d, 2 * d)

    def pre_span(i):
        return pl.ds(pl.multiple_of(i * pre_chunk, pre_chunk), pre_chunk)

    def ans_span(i):
        return pl.ds(pl.multiple_of(pre_total + i * ans_chunk, ans_chunk), ans_chunk)

    def fold(values, into):
        return jnp.maximum(into, jnp.max(values.reshape(values.shape[0] // 8, 8, rows), axis=0))

    @pl.when(live_here)
    def _():
        place_rows = lax.broadcasted_iota(jnp.int32, (ans_here, d), 0)
        alive = place_rows + first_row < length
        for g in range(group):
            lanes = slice(g * d, (g + 1) * d)
            here = slice(g * ans_here, (g + 1) * ans_here)
            queries[here] = q_ref[0, :, lanes]
            douts[here] = jnp.where(alive, g_ref[0, :, lanes].astype(F32), 0.0)
        douts_t[...] = douts[...].T
        top[...] = jnp.full_like(top, NEGATIVE)

        def score(i, block, span, keep):
            values = nt(block(i, keys_at), queries[...])
            if keep is not None:
                values = jnp.where(keep(i, values.shape), values, NEGATIVE)
            scores[span(i)] = values
            top[...] = fold(values, top[...])

        def pre_keep(i, shape):
            return lax.broadcasted_iota(jnp.int32, shape, 0) + i * pre_chunk < limit

        def ans_keep(i, shape):
            key = lax.broadcasted_iota(jnp.int32, shape, 0) + i * ans_chunk
            row = lax.broadcasted_iota(jnp.int32, shape, 1) % ans_here + first_row
            return key <= row

        @pl.loop(0, n_full)
        def _(i):
            score(i, pre_block, pre_span, None)

        @pl.when(n_full < n_pre)
        def _():
            score(n_full, pre_block, pre_span, pre_keep)

        @pl.loop(0, n_ans - 1)
        def _(i):
            score(i, ans_block, ans_span, None)

        score(n_ans - 1, ans_block, ans_span, ans_keep)

        top_row = jnp.max(top[...], axis=0, keepdims=True)
        shift = top_row * (scale * LOG2E)
        row_sum[...] = jnp.zeros_like(row_sum)
        acc_t[...] = jnp.zeros_like(acc_t)

        def spread(i, block, span):
            e = jnp.exp2(scores[span(i)] * (scale * LOG2E) - shift)
            row_sum[...] += jnp.sum(e.reshape(e.shape[0] // 8, 8, rows), axis=0)
            low = e.astype(BF16)
            weights[span(i)] = low
            acc_t[...] += nn(block(i, values_at).T, low)

        @pl.loop(0, n_pre)
        def _(i):
            spread(i, pre_block, pre_span)

        @pl.loop(0, n_ans)
        def _(i):
            spread(i, ans_block, ans_span)

        inverse = 1.0 / jnp.sum(row_sum[...], axis=0, keepdims=True)
        attended_t = acc_t[...] * inverse
        scaled = (douts_t[...] * inverse).astype(BF16)
        delta = jnp.sum(scaled.astype(F32) * attended_t, axis=0, keepdims=True)
        douts_low_t = scaled
        queries_t[...] = douts_low_t
        douts_low = douts_low_t.astype(F32).T.astype(BF16)
        attended = attended_t.T
        for g in range(group):
            lanes = slice(g * d, (g + 1) * d)
            here = slice(g * ans_here, (g + 1) * ans_here)
            out_ref[0, :, lanes] = jnp.where(alive, attended[here], 0.0).astype(BF16)
        douts[...] = douts_low.astype(F32)
        acc_t[...] = jnp.zeros_like(acc_t)

        def back(i, block, span):
            low = weights[span(i)]
            grad_probs = nn(block(i, values_at), queries_t[...])
            grad_low = (low.astype(F32) * (grad_probs - delta)).astype(BF16)
            value_term = nn(low, douts_low)
            key_term = nn(grad_low, queries[...]) * scale
            acc_t[...] += nn(block(i, keys_at).T, grad_low)
            return key_term, value_term

        @pl.loop(0, n_pre)
        def _(i):
            key_term, value_term = back(i, pre_block, pre_span)
            prefix_terms[pre_span(i), 0:d] += key_term
            prefix_terms[pre_span(i), d : 2 * d] += value_term

        @pl.loop(0, n_ans)
        def _(i):
            key_term, value_term = back(i, ans_block, ans_span)
            at = pl.ds(i * ANS_SOURCES, ANS_SOURCES)
            span = pl.ds(ans_at, ans_here)
            terms_ref[0, at, span, 0:d] = key_term.astype(BF16).reshape(ANS_SOURCES, ans_here, d)
            terms_ref[0, at, span, d : 2 * d] = value_term.astype(BF16).reshape(ANS_SOURCES, ans_here, d)

        grad_queries = (acc_t[...] * scale).T
        for g in range(group):
            lanes = slice(g * d, (g + 1) * d)
            here = slice(g * ans_here, (g + 1) * ans_here)
            dq_ref[0, :, lanes] = grad_queries[here].astype(BF16)

    @pl.when(jnp.logical_not(live_here))
    def _():
        out_ref[...] = jnp.zeros_like(out_ref)
        dq_ref[...] = jnp.zeros_like(dq_ref)

    @pl.when(b == 1)
    def _():
        @pl.loop(0, 2 * per_pair)
        def _(i):
            pair_at, source = i // per_pair, (i % per_pair) * PRE_SOURCES
            row = pl.multiple_of(2 * ans_here + pair_at * pre_rows, 16)
            terms_ref[0, pl.ds(source, PRE_SOURCES), pl.ds(row, pre_rows), :] = (
                prefix_terms[pre_span(i)].astype(BF16).reshape(PRE_SOURCES, pre_rows, 2 * d)
            )


def attend(queries, grad_out, gathered, lengths, limits, ans_here, pre_rows):
    batch, _, features = queries.shape
    kv, sources, rows_all, width = gathered.shape
    d = HEAD_DIM
    group = features // d // kv
    keys_total = sources * ans_here + 2 * sources * pre_rows
    rows = group * ans_here
    query_spec = pl.BlockSpec((1, ans_here, group * d), lambda c, b: (b, 0, c))
    kv_spec = pl.BlockSpec((1, sources, rows_all, width), lambda c, b: (c, 0, 0, 0))
    smem = pl.BlockSpec(memory_space=pltpu.SMEM)
    return pl.pallas_call(
        functools.partial(attend_kernel, ans_here, pre_rows, group),
        grid=(kv, batch),
        out_shape=(
            jax.ShapeDtypeStruct(queries.shape, BF16),
            jax.ShapeDtypeStruct(queries.shape, BF16),
            jax.ShapeDtypeStruct(gathered.shape, BF16),
        ),
        in_specs=[smem, smem, query_spec, query_spec, kv_spec],
        out_specs=(query_spec, query_spec, kv_spec),
        scratch_shapes=[
            pltpu.VMEM((keys_total, rows), F32),
            pltpu.VMEM((keys_total, rows), BF16),
            pltpu.VMEM((rows, d), BF16),
            pltpu.VMEM((rows, d), F32),
            pltpu.VMEM((d, rows), BF16),
            pltpu.VMEM((d, rows), F32),
            pltpu.VMEM((2 * sources * pre_rows, width), F32),
            pltpu.VMEM((8, rows), F32),
            pltpu.VMEM((8, rows), F32),
            pltpu.VMEM((d, rows), F32),
        ],
        compiler_params=pltpu.CompilerParams(
            dimension_semantics=("arbitrary", "arbitrary"), vmem_limit_bytes=60 * 1024 * 1024
        ),
        name="attend",
    )(lengths, limits, queries, grad_out, gathered)


def on_device(
    queries,
    answer_keys,
    answer_values,
    prefix_keys,
    prefix_values,
    grad_out,
    answer_length,
    prefix_limit,
):
    d = HEAD_DIM
    _, ans_here, batch, features = queries.shape
    kv = answer_keys.shape[3] // d
    pre_rows = prefix_keys.shape[0]
    side = lax.axis_size("seq")

    def by_head(keys, values):
        both = jnp.stack([keys.reshape(-1, kv, d), values.reshape(-1, kv, d)], axis=2)
        return both.transpose(1, 0, 2, 3).reshape(kv, -1, 2 * d)

    def batch_first(x):
        return x[0].transpose(1, 0, 2)

    ans = by_head(batch_first(answer_keys), batch_first(answer_values))
    pre = by_head(prefix_keys, prefix_values)
    gathered = gather(ans, pre)
    flat = gathered.reshape(kv, side, gathered.shape[-2], 2 * d)
    out, grad_queries, terms = attend(
        batch_first(queries), batch_first(grad_out), flat, answer_length, prefix_limit, ans_here, pre_rows
    )
    ans_sums, pre_sums = scatter(terms.reshape(gathered.shape), batch * ans_here, pre_rows)

    def back(x):
        return x.transpose(1, 0, 2)[None]

    def apart(x, n):
        return x[:, :, n * d : (n + 1) * d]

    def ans_grad(n):
        x = apart(ans_sums, n).reshape(kv, batch, ans_here, d).transpose(2, 1, 0, 3)
        return x.reshape(answer_keys.shape)

    def pre_grad(n):
        return apart(pre_sums, n).transpose(1, 0, 2).reshape(prefix_keys.shape)

    return (back(out), back(grad_queries), ans_grad(0), ans_grad(1), pre_grad(0), pre_grad(1))


def solution(mesh):
    tokens = P("pair", "seq", None, "head")
    prefix = P(("pair", "seq"), "head")
    scalars = P("pair", None)
    return jax.shard_map(
        on_device,
        mesh=mesh,
        in_specs=(tokens, tokens, tokens, prefix, prefix, tokens, scalars, scalars),
        out_specs=(tokens, tokens, tokens, tokens, prefix, prefix),
        check_vma=False,
    )
```

```python
import functools

import jax
import jax.numpy as jnp
from jax import lax
from jax.experimental import pallas as pl
from jax.experimental.pallas import tpu as pltpu
from jax.sharding import PartitionSpec as P

HEAD_DIM = 128
RING = 4
CORES = 2
LOG2E = 1.4426950408889634
NEGATIVE = -1e30
MESH = pl.DeviceIdType.MESH
BF16 = jnp.bfloat16
F32 = jnp.float32


def place():
    s = lax.axis_index("seq")
    return s // (RING * CORES), (s // CORES) % RING, s % CORES


def seq_of(z, y, core):
    return (z * RING + y) * CORES + core


def shifted(h, dp, dq):
    z, y, _ = place()
    return (z + dp * h + dq * (1 - h)) % RING, (y + dp * (1 - h) + dq * h) % RING


def to(h, dp, dq):
    z, y = shifted(h, dp, dq)
    return {"seq": seq_of(z, y, place()[2])}


def across(same_core):
    z, y, core = place()
    target = {"pair": 1 - lax.axis_index("pair")}
    if not same_core:
        target["seq"] = seq_of(z, y, 1 - core)
    return target


def sibling():
    z, y, core = place()
    return {"seq": seq_of(z, y, 1 - core)}


def greet():
    barrier = pltpu.get_barrier_semaphore()
    peers = [to(h, d, 0) for h in range(2) for d in (1, RING - 1)]
    peers += [sibling(), across(True), across(False)]
    for peer in peers:
        pl.semaphore_signal(barrier, inc=1, device_id=peer, device_id_type=MESH)
    pl.semaphore_wait(barrier, len(peers))


def spans(ans_rows, pre_rows):
    pair = lax.axis_index("pair")
    rows = ans_rows + 2 * pre_rows
    half = rows // 2
    parts = (pl.ds(0, half), pl.ds(half, rows - half))
    mine = pl.ds(pl.multiple_of(ans_rows + pair * pre_rows, 16), pre_rows)
    other = pl.ds(pl.multiple_of(ans_rows + (1 - pair) * pre_rows, 16), pre_rows)
    return rows, parts, mine, other


class Copies:
    def __init__(self, send_sem, recv_sem):
        self.send_sem, self.recv_sem = send_sem, recv_sem
        self.ids = {}
        self.sent = []

    def make(self, key, src, dst, to):
        n = self.ids.setdefault(key, len(self.ids))
        return pltpu.make_async_remote_copy(
            src_ref=src,
            dst_ref=dst,
            send_sem=self.send_sem.at[n],
            recv_sem=self.recv_sem.at[n],
            device_id=to,
            device_id_type=MESH,
        )

    def send(self, key, src, dst, to):
        copy = self.make(key, src, dst, to)
        copy.start()
        self.sent.append(copy)

    def arrived(self, key, dst, to):
        self.make(key, dst, dst, to).wait_recv()

    def finish(self):
        for copy in self.sent:
            copy.wait_send()


ORDER = (0, 3, 1, 2)
GATHER_COPIES = 80


def gather_kernel(
    ans_rows, pre_rows, ans_ref, pre_ref, q_ref, g_ref, kv_out, q_out, g_out, held, send_sem, recv_sem, local_sem, out_sem
):
    z, y, core = place()
    rows, parts, mine, other = spans(ans_rows, pre_rows)
    pieces = (pl.ds(0, ans_rows), pl.ds(ans_rows, 2 * pre_rows))
    copies = Copies(send_sem, recv_sem)
    sources = (core, 1 - core)
    stores = []

    def block(r, dp, dq):
        zz, yy = shifted(sources[r], dp, dq)
        return held.at[zz, yy, sources[r]]

    pos = q_ref.shape[2]
    own_rows = pl.ds(pl.multiple_of(core * pos, pos), pos)
    sibling_rows = pl.ds(pl.multiple_of((1 - core) * pos, pos), pos)
    loads = [
        pltpu.make_async_copy(ans_ref.at[core], block(0, 0, 0).at[pieces[0]], local_sem.at[0]),
        pltpu.make_async_copy(pre_ref.at[core], block(0, 0, 0).at[mine], local_sem.at[1]),
        pltpu.make_async_copy(q_ref.at[core], q_out.at[:, own_rows], local_sem.at[2]),
        pltpu.make_async_copy(g_ref.at[core], g_out.at[:, own_rows], local_sem.at[3]),
    ]
    for copy in loads:
        copy.start()
    greet()
    there = held.at[z, y, core]
    copies.send(("sib", 0), ans_ref.at[1 - core], there.at[pieces[0]], sibling())
    copies.send(("sib", 1), pre_ref.at[1 - core], there.at[mine], sibling())
    copies.send(("pair", 0), pre_ref.at[core], there.at[mine], across(True))
    copies.send(("pair", 1), pre_ref.at[1 - core], there.at[mine], across(False))

    def pass_on(key, r, ref, axis, direction):
        target = to(sources[r], direction, 0) if axis == 0 else to(sources[r], 0, direction)
        copies.send(key, ref, ref, target)

    def own(r, piece):
        ref = block(r, 0, 0).at[pieces[piece]]
        for direction in (1, 3):
            pass_on(("one", r, direction, piece), r, ref, 0, direction)
        for direction in (1, 3):
            pass_on(("two", r, 0, direction, piece), r, ref, 1, direction)

    def spread(r, k):
        for direction in (1, 3):
            pass_on(("two", r, k, direction, 2), r, block(r, ORDER[k], 0), 1, direction)

    def keep(r, dp, dq):
        zz, yy = shifted(sources[r], dp, dq)
        store = pltpu.make_async_copy(
            held.at[zz, yy, sources[r]], kv_out.at[zz, yy, sources[r]], out_sem.at[len(stores)]
        )
        store.start()
        stores.append(store)

    loads[0].wait()
    own(0, 0)
    copies.arrived(("sib", 0), block(1, 0, 0).at[pieces[0]], sibling())
    own(1, 0)
    loads[1].wait()
    copies.arrived(("pair", 0), block(0, 0, 0).at[other], across(True))
    own(0, 1)
    keep(0, 0, 0)
    copies.arrived(("sib", 1), block(1, 0, 0).at[mine], sibling())
    copies.arrived(("pair", 1), block(1, 0, 0).at[other], across(False))
    own(1, 1)
    keep(1, 0, 0)
    copies.send(("sib", 2), q_ref.at[1 - core], q_out.at[:, own_rows], sibling())
    copies.send(("sib", 3), g_ref.at[1 - core], g_out.at[:, own_rows], sibling())

    for direction in (1, 3):
        for r in range(2):
            back = (-direction) % RING
            for piece in range(2):
                copies.arrived(
                    ("one", r, direction, piece), block(r, back, 0).at[pieces[piece]], to(sources[r], direction, 0)
                )
            n = direction // 2
            pass_on(("far", r, direction), r, block(r, back, 0).at[parts[n]], 0, direction)
            spread(r, ORDER.index(back))
            keep(r, back, 0)
    for r in range(2):
        for direction in (1, 3):
            copies.arrived(
                ("far", r, direction), block(r, 2, 0).at[parts[direction // 2]], to(sources[r], direction, 0)
            )
        spread(r, 3)
        keep(r, 2, 0)
    for k in range(RING):
        for direction in (1, 3):
            for r in range(2):
                back = (-direction) % RING
                here = block(r, ORDER[k], back)
                for piece in range(2) if k == 0 else (2,):
                    area = here if piece == 2 else here.at[pieces[piece]]
                    copies.arrived(("two", r, k, direction, piece), area, to(sources[r], 0, direction))
                pass_on(("far2", r, k, direction), r, here.at[parts[direction // 2]], 1, direction)
                keep(r, ORDER[k], back)
    for k in range(RING):
        for r in range(2):
            here = block(r, ORDER[k], 2)
            for direction in (1, 3):
                copies.arrived(("far2", r, k, direction), here.at[parts[direction // 2]], to(sources[r], 0, direction))
            keep(r, ORDER[k], 2)
    copies.arrived(("sib", 2), q_out.at[:, sibling_rows], sibling())
    copies.arrived(("sib", 3), g_out.at[:, sibling_rows], sibling())
    loads[2].wait()
    loads[3].wait()
    for store in stores:
        store.wait()
    copies.finish()


def gather(ans, pre, queries, grad_out):
    _, ans_rows, width = ans.shape
    pre_rows = pre.shape[1]
    rows = ans_rows + 2 * pre_rows
    _, batch, pos, features = queries.shape
    anywhere = pl.BlockSpec(memory_space=pl.ANY)
    both = jax.ShapeDtypeStruct((batch, CORES * pos, features), queries.dtype)
    return pl.pallas_call(
        functools.partial(gather_kernel, ans_rows, pre_rows),
        out_shape=(jax.ShapeDtypeStruct((RING, RING, CORES, rows, width), ans.dtype), both, both),
        in_specs=[pl.BlockSpec(memory_space=pltpu.VMEM)] * 4,
        out_specs=(anywhere, anywhere, anywhere),
        scratch_shapes=[
            pltpu.VMEM((RING, RING, CORES, rows, width), ans.dtype),
            pltpu.SemaphoreType.DMA((GATHER_COPIES,)),
            pltpu.SemaphoreType.DMA((GATHER_COPIES,)),
            pltpu.SemaphoreType.DMA((4,)),
            pltpu.SemaphoreType.DMA((2 * RING * RING,)),
        ],
        compiler_params=pltpu.CompilerParams(collective_id=0, has_side_effects=True),
        name="gather",
    )(ans, pre, queries, grad_out)


SCATTER_COPIES = 60


def scatter_kernel(
    ans_rows,
    pre_rows,
    terms_ref,
    att_ref,
    dq_ref,
    ans_out,
    pre_out,
    att_out,
    dq_out,
    total,
    far2,
    near2,
    far1,
    near1,
    ans_swap,
    pre_swap,
    pre_got,
    send_sem,
    recv_sem,
    local_sem,
    out_sem,
):
    z, y, core = place()
    rows, parts, mine, other = spans(ans_rows, pre_rows)
    copies = Copies(send_sem, recv_sem)
    sources = (core, 1 - core)
    order = (2, 1, 3, 0)
    q_order = (2, 1, 3, 0)

    def block(r, dp, dq):
        zz, yy = shifted(sources[r], dp, dq)
        return total.at[zz, yy, sources[r]]

    loads = {}
    for k in range(RING):
        for r in range(2):
            for m in range(RING):
                zz, yy = shifted(sources[r], order[k], q_order[m])
                spot = (zz, yy, sources[r])
                n = len(loads)
                loads[r, k, m] = pltpu.make_async_copy(terms_ref.at[spot], total.at[spot], local_sem.at[n])
                loads[r, k, m].start()
    pos = att_ref.shape[1] // CORES
    own_rows = pl.ds(pl.multiple_of(core * pos, pos), pos)
    sibling_rows = pl.ds(pl.multiple_of((1 - core) * pos, pos), pos)
    greet()
    for k in range(RING):
        for r in range(2):
            loads[r, k, 0].wait()
            for n, direction in enumerate((1, 3)):
                copies.send(
                    ("far2", r, k, n),
                    block(r, order[k], 2).at[parts[n]],
                    far2.at[r, k, n],
                    to(sources[r], 0, direction),
                )
    outs = [
        pltpu.make_async_copy(att_ref.at[:, own_rows], att_out.at[core], out_sem.at[0]),
        pltpu.make_async_copy(dq_ref.at[:, own_rows], dq_out.at[core], out_sem.at[1]),
    ]
    for copy in outs:
        copy.start()
    copies.send(("sib", 0), att_ref.at[:, sibling_rows], att_out.at[core], sibling())
    copies.send(("sib", 1), dq_ref.at[:, sibling_rows], dq_out.at[core], sibling())

    def add(into, other_ref):
        into[...] = (into[...].astype(F32) + other_ref[...].astype(F32)).astype(BF16)

    for k in range(RING):
        for r in range(2):
            for n, direction in enumerate((1, 3)):
                loads[r, k, 1 + n].wait()
                here = block(r, order[k], direction)
                copies.arrived(("far2", r, k, n), far2.at[r, k, n], to(sources[r], 0, direction))
                add(here.at[parts[n]], far2.at[r, k, n])
                copies.send(("near2", r, k, n), here, near2.at[r, k, n], to(sources[r], 0, direction))

    def settle2(r, k):
        loads[r, k, 3].wait()
        for n, direction in enumerate((1, 3)):
            copies.arrived(("near2", r, k, n), near2.at[r, k, n], to(sources[r], 0, direction))
        into = block(r, order[k], 0)
        into[...] = (
            into[...].astype(F32) + near2[r, k, 0].astype(F32) + near2[r, k, 1].astype(F32)
        ).astype(BF16)

    for r in range(2):
        settle2(r, 0)
        for n, direction in enumerate((1, 3)):
            copies.send(("far1", r, n), block(r, 2, 0).at[parts[n]], far1.at[r, n], to(sources[r], direction, 0))
    for k in (1, 2):
        n = k - 1
        direction = order[k]
        for r in range(2):
            settle2(r, k)
            here = block(r, direction, 0)
            copies.arrived(("far1", r, n), far1.at[r, n], to(sources[r], direction, 0))
            add(here.at[parts[n]], far1.at[r, n])
            copies.send(("near1", r, n), here, near1.at[r, n], to(sources[r], direction, 0))
    for r in range(2):
        settle2(r, 3)
    for r in (1, 0):
        for n, direction in enumerate((1, 3)):
            copies.arrived(("near1", r, n), near1.at[r, n], to(sources[r], direction, 0))
        here = block(r, 0, 0)

        def final(area):
            return (
                here[area].astype(F32) + near1[r, 0, area].astype(F32) + near1[r, 1, area].astype(F32)
            )

        pre_swap[r, 0] = final(other).astype(BF16)
        if r == 1:
            copies.send(("pre", 1, 0), pre_swap.at[1, 0], pre_got.at[1, 0], across(False))
            pre_swap[1, 1] = final(mine).astype(BF16)
            copies.send(("pre", 1, 1), pre_swap.at[1, 1], pre_got.at[1, 1], sibling())
            ans_swap[...] = final(pl.ds(0, ans_rows)).astype(BF16)
            copies.send(("ans",), ans_swap, ans_out.at[core], sibling())
        else:
            copies.send(("pre", 0, 0), pre_swap.at[0, 0], pre_got.at[0, 0], across(True))
            pre_out[core] = final(mine)
            ans_out[core] = final(pl.ds(0, ans_rows)).astype(BF16)
    copies.arrived(("pre", 1, 1), pre_got.at[1, 1], sibling())
    copies.arrived(("pre", 1, 0), pre_got.at[1, 0], across(False))
    pre_out[1 - core] = pre_got[1, 0].astype(F32) + pre_got[1, 1].astype(F32)
    copies.arrived(("pre", 0, 0), pre_got.at[0, 0], across(True))
    pre_out[core] = pre_out[core] + pre_got[0, 0].astype(F32)
    copies.arrived(("ans",), ans_out.at[1 - core], sibling())
    copies.arrived(("sib", 0), att_out.at[1 - core], sibling())
    copies.arrived(("sib", 1), dq_out.at[1 - core], sibling())
    for copy in outs:
        copy.wait()
    copies.finish()


def scatter(terms, attended, grad_queries, ans_rows, pre_rows):
    rows, width = terms.shape[-2:]
    half = rows // 2
    batch, pos2, features = attended.shape
    split = jax.ShapeDtypeStruct((CORES, batch, pos2 // CORES, features), attended.dtype)
    vmem = pl.BlockSpec(memory_space=pltpu.VMEM)
    anywhere = pl.BlockSpec(memory_space=pl.ANY)
    return pl.pallas_call(
        functools.partial(scatter_kernel, ans_rows, pre_rows),
        out_shape=(
            jax.ShapeDtypeStruct((CORES, ans_rows, width), BF16),
            jax.ShapeDtypeStruct((CORES, pre_rows, width), F32),
            split,
            split,
        ),
        in_specs=[anywhere, vmem, vmem],
        out_specs=(vmem, vmem, anywhere, anywhere),
        scratch_shapes=[
            pltpu.VMEM((RING, RING, CORES, rows, width), BF16),
            pltpu.VMEM((CORES, RING, 2, half, width), BF16),
            pltpu.VMEM((CORES, RING, 2, rows, width), BF16),
            pltpu.VMEM((CORES, 2, half, width), BF16),
            pltpu.VMEM((CORES, 2, rows, width), BF16),
            pltpu.VMEM((ans_rows, width), BF16),
            pltpu.VMEM((2, 2, pre_rows, width), BF16),
            pltpu.VMEM((2, 2, pre_rows, width), BF16),
            pltpu.SemaphoreType.DMA((SCATTER_COPIES,)),
            pltpu.SemaphoreType.DMA((SCATTER_COPIES,)),
            pltpu.SemaphoreType.DMA((2 * RING * RING,)),
            pltpu.SemaphoreType.DMA((2,)),
        ],
        compiler_params=pltpu.CompilerParams(collective_id=1, has_side_effects=True),
        name="scatter",
    )(terms, attended, grad_queries)


def nn(a, b):
    return lax.dot_general(a, b, (((1,), (0,)), ((), ())), preferred_element_type=F32)


def nt(a, b):
    return lax.dot_general(a, b, (((1,), (1,)), ((), ())), preferred_element_type=F32)


ANS_SOURCES = 4
PRE_SOURCES = 8


def attend_kernel(
    ans_here,
    pre_rows,
    group,
    length_ref,
    limit_ref,
    q_ref,
    g_ref,
    kv_ref,
    out_ref,
    dq_ref,
    terms_ref,
    scores,
    weights,
    queries,
    douts,
    queries_t,
    douts_t,
    prefix_terms,
    top,
    row_sum,
    acc_t,
):
    sources = kv_ref.shape[0]
    d = HEAD_DIM
    b = pl.program_id(0)
    s = lax.axis_index("seq")
    scale = d**-0.5
    here_rows = CORES * ans_here
    rows = group * here_rows
    ans_chunk = ANS_SOURCES * ans_here
    pre_chunk = PRE_SOURCES * pre_rows
    per_pair = sources // PRE_SOURCES
    pre_total = 2 * sources * pre_rows
    first_row = (s // CORES) * here_rows
    length = length_ref[0, b]
    limit = limit_ref[0, b]
    ans_at = pl.multiple_of(b * ans_here, ans_here)
    live_here = first_row < length
    n_pre = jnp.where(live_here, (limit + pre_chunk - 1) // pre_chunk, 0)
    n_full = jnp.where(live_here, limit // pre_chunk, 0)
    n_ans = jnp.where(live_here, (s // CORES) * CORES // ANS_SOURCES + 1, 0)

    @pl.when(b == 0)
    def _():
        prefix_terms[...] = jnp.zeros_like(prefix_terms)

    terms_ref[:, pl.ds(ans_at, ans_here), :] = jnp.zeros((sources, ans_here, 2 * d), BF16)

    def pre_block(i, lanes):
        pair_at, source = i // per_pair, (i % per_pair) * PRE_SOURCES
        row = pl.multiple_of(2 * ans_here + pair_at * pre_rows, 16)
        part = kv_ref[pl.ds(source, PRE_SOURCES), pl.ds(row, pre_rows), lanes]
        return part.reshape(pre_chunk, d)

    def ans_block(i, lanes):
        part = kv_ref[pl.ds(i * ANS_SOURCES, ANS_SOURCES), pl.ds(ans_at, ans_here), lanes]
        return part.reshape(ans_chunk, d)

    keys_at, values_at = slice(0, d), slice(d, 2 * d)

    def pre_span(i):
        return pl.ds(pl.multiple_of(i * pre_chunk, pre_chunk), pre_chunk)

    def ans_span(i):
        return pl.ds(pl.multiple_of(pre_total + i * ans_chunk, ans_chunk), ans_chunk)

    def fold(values, into):
        return jnp.maximum(into, jnp.max(values.reshape(values.shape[0] // 8, 8, rows), axis=0))

    @pl.when(live_here)
    def _():
        place_rows = lax.broadcasted_iota(jnp.int32, (here_rows, d), 0)
        alive = place_rows + first_row < length
        for g in range(group):
            lanes = slice(g * d, (g + 1) * d)
            here = slice(g * here_rows, (g + 1) * here_rows)
            queries[here] = q_ref[0, :, lanes]
            douts[here] = jnp.where(alive, g_ref[0, :, lanes].astype(F32), 0.0)
        douts_t[...] = douts[...].T
        top[...] = jnp.full_like(top, NEGATIVE)

        def score(i, block, span, keep):
            values = nt(block(i, keys_at), queries[...])
            if keep is not None:
                values = jnp.where(keep(i, values.shape), values, NEGATIVE)
            scores[span(i)] = values
            top[...] = fold(values, top[...])

        def pre_keep(i, shape):
            return lax.broadcasted_iota(jnp.int32, shape, 0) + i * pre_chunk < limit

        def ans_keep(i, shape):
            key = lax.broadcasted_iota(jnp.int32, shape, 0) + i * ans_chunk
            row = lax.broadcasted_iota(jnp.int32, shape, 1) % here_rows + first_row
            return key <= row

        @pl.loop(0, n_full)
        def _(i):
            score(i, pre_block, pre_span, None)

        @pl.when(n_full < n_pre)
        def _():
            score(n_full, pre_block, pre_span, pre_keep)

        @pl.loop(0, n_ans - 1)
        def _(i):
            score(i, ans_block, ans_span, None)

        score(n_ans - 1, ans_block, ans_span, ans_keep)

        top_row = jnp.max(top[...], axis=0, keepdims=True)
        shift = top_row * (scale * LOG2E)
        row_sum[...] = jnp.zeros_like(row_sum)
        acc_t[...] = jnp.zeros_like(acc_t)

        def spread(i, block, span):
            e = jnp.exp2(scores[span(i)] * (scale * LOG2E) - shift)
            row_sum[...] += jnp.sum(e.reshape(e.shape[0] // 8, 8, rows), axis=0)
            low = e.astype(BF16)
            weights[span(i)] = low
            acc_t[...] += nn(block(i, values_at).T, low)

        @pl.loop(0, n_pre)
        def _(i):
            spread(i, pre_block, pre_span)

        @pl.loop(0, n_ans)
        def _(i):
            spread(i, ans_block, ans_span)

        inverse = 1.0 / jnp.sum(row_sum[...], axis=0, keepdims=True)
        attended_t = acc_t[...] * inverse
        scaled = (douts_t[...] * inverse).astype(BF16)
        delta = jnp.sum(scaled.astype(F32) * attended_t, axis=0, keepdims=True)
        douts_low_t = scaled
        queries_t[...] = douts_low_t
        douts_low = douts_low_t.astype(F32).T.astype(BF16)
        attended = attended_t.T
        for g in range(group):
            lanes = slice(g * d, (g + 1) * d)
            here = slice(g * here_rows, (g + 1) * here_rows)
            out_ref[0, :, lanes] = jnp.where(alive, attended[here], 0.0).astype(BF16)
        douts[...] = douts_low.astype(F32)
        acc_t[...] = jnp.zeros_like(acc_t)

        def back(i, block, span):
            low = weights[span(i)]
            grad_probs = nn(block(i, values_at), queries_t[...])
            grad_low = (low.astype(F32) * (grad_probs - delta)).astype(BF16)
            value_term = nn(low, douts_low)
            key_term = nn(grad_low, queries[...]) * scale
            acc_t[...] += nn(block(i, keys_at).T, grad_low)
            return key_term, value_term

        @pl.loop(0, n_pre)
        def _(i):
            key_term, value_term = back(i, pre_block, pre_span)
            prefix_terms[pre_span(i), 0:d] += key_term
            prefix_terms[pre_span(i), d : 2 * d] += value_term

        @pl.loop(0, n_ans)
        def _(i):
            key_term, value_term = back(i, ans_block, ans_span)
            at = pl.ds(i * ANS_SOURCES, ANS_SOURCES)
            span = pl.ds(ans_at, ans_here)
            terms_ref[at, span, 0:d] = key_term.astype(BF16).reshape(ANS_SOURCES, ans_here, d)
            terms_ref[at, span, d : 2 * d] = value_term.astype(BF16).reshape(ANS_SOURCES, ans_here, d)

        grad_queries = (acc_t[...] * scale).T
        for g in range(group):
            lanes = slice(g * d, (g + 1) * d)
            here = slice(g * here_rows, (g + 1) * here_rows)
            dq_ref[0, :, lanes] = grad_queries[here].astype(BF16)

    @pl.when(jnp.logical_not(live_here))
    def _():
        out_ref[...] = jnp.zeros_like(out_ref)
        dq_ref[...] = jnp.zeros_like(dq_ref)

    @pl.when(b == 1)
    def _():
        @pl.loop(0, 2 * per_pair)
        def _(i):
            pair_at, source = i // per_pair, (i % per_pair) * PRE_SOURCES
            row = pl.multiple_of(2 * ans_here + pair_at * pre_rows, 16)
            terms_ref[pl.ds(source, PRE_SOURCES), pl.ds(row, pre_rows), :] = (
                prefix_terms[pre_span(i)].astype(BF16).reshape(PRE_SOURCES, pre_rows, 2 * d)
            )


def attend(queries, grad_out, gathered, lengths, limits, ans_here, pre_rows):
    batch, here_rows, features = queries.shape
    sources, rows_all, width = gathered.shape
    d = HEAD_DIM
    group = features // d
    keys_total = sources * ans_here + 2 * sources * pre_rows
    rows = group * here_rows
    query_spec = pl.BlockSpec((1, here_rows, features), lambda b: (b, 0, 0))
    kv_spec = pl.BlockSpec((sources, rows_all, width), lambda b: (0, 0, 0))
    smem = pl.BlockSpec(memory_space=pltpu.SMEM)
    return pl.pallas_call(
        functools.partial(attend_kernel, ans_here, pre_rows, group),
        grid=(batch,),
        out_shape=(
            jax.ShapeDtypeStruct(queries.shape, BF16),
            jax.ShapeDtypeStruct(queries.shape, BF16),
            jax.ShapeDtypeStruct(gathered.shape, BF16),
        ),
        in_specs=[smem, smem, query_spec, query_spec, kv_spec],
        out_specs=(query_spec, query_spec, kv_spec),
        scratch_shapes=[
            pltpu.VMEM((keys_total, rows), F32),
            pltpu.VMEM((keys_total, rows), BF16),
            pltpu.VMEM((rows, d), BF16),
            pltpu.VMEM((rows, d), F32),
            pltpu.VMEM((d, rows), BF16),
            pltpu.VMEM((d, rows), F32),
            pltpu.VMEM((2 * sources * pre_rows, width), F32),
            pltpu.VMEM((8, rows), F32),
            pltpu.VMEM((8, rows), F32),
            pltpu.VMEM((d, rows), F32),
        ],
        compiler_params=pltpu.CompilerParams(
            dimension_semantics=("arbitrary",), vmem_limit_bytes=60 * 1024 * 1024
        ),
        name="attend",
    )(lengths, limits, queries, grad_out, gathered)


def on_device(
    queries,
    answer_keys,
    answer_values,
    prefix_keys,
    prefix_values,
    grad_out,
    answer_length,
    prefix_limit,
):
    d = HEAD_DIM
    _, ans_here, batch, features = queries.shape
    kv = answer_keys.shape[3] // d
    pre_rows = prefix_keys.shape[0]
    side = lax.axis_size("seq")

    def by_head(keys, values):
        both = jnp.stack([keys.reshape(-1, kv, d), values.reshape(-1, kv, d)], axis=2)
        return both.transpose(1, 0, 2, 3).reshape(kv, -1, 2 * d)

    def batch_first(x):
        return x[0].transpose(1, 0, 2)

    def head_first(x):
        return x[0].reshape(ans_here, batch, kv, features // kv).transpose(2, 1, 0, 3)

    ans = by_head(batch_first(answer_keys), batch_first(answer_values))
    pre = by_head(prefix_keys, prefix_values)
    gathered, q_here, g_here = gather(ans, pre, head_first(queries), head_first(grad_out))
    flat = gathered.reshape(side, gathered.shape[-2], 2 * d)
    attended, grad_q, terms = attend(q_here, g_here, flat, answer_length, prefix_limit, ans_here, pre_rows)
    ans_sums, pre_sums, out, grad_queries = scatter(
        terms.reshape(gathered.shape), attended, grad_q, batch * ans_here, pre_rows
    )

    def back(x):
        return x.transpose(2, 1, 0, 3).reshape(queries.shape)

    def apart(x, n):
        return x[:, :, n * d : (n + 1) * d]

    def ans_grad(n):
        x = apart(ans_sums, n).reshape(kv, batch, ans_here, d).transpose(2, 1, 0, 3)
        return x.reshape(answer_keys.shape)

    def pre_grad(n):
        return apart(pre_sums, n).transpose(1, 0, 2).reshape(prefix_keys.shape)

    return (back(out), back(grad_queries), ans_grad(0), ans_grad(1), pre_grad(0), pre_grad(1))


def solution(mesh):
    tokens = P("pair", "seq", None, "head")
    prefix = P(("pair", "seq"), "head")
    scalars = P("pair", None)
    return jax.shard_map(
        on_device,
        mesh=mesh,
        in_specs=(tokens, tokens, tokens, prefix, prefix, tokens, scalars, scalars),
        out_specs=(tokens, tokens, tokens, tokens, prefix, prefix),
        check_vma=False,
    )
```

```python
import functools

import jax
import jax.numpy as jnp
from jax import lax
from jax.experimental import pallas as pl
from jax.experimental.pallas import tpu as pltpu
from jax.sharding import PartitionSpec as P

HEAD_DIM = 128
RING = 4
CORES = 2
LOG2E = 1.4426950408889634
NEGATIVE = -1e30
MESH = pl.DeviceIdType.MESH
BF16 = jnp.bfloat16
F32 = jnp.float32


def place():
    s = lax.axis_index("seq")
    return s // (RING * CORES), (s // CORES) % RING, s % CORES


def seq_of(z, y, core):
    return (z * RING + y) * CORES + core


def shifted(h, dp, dq):
    z, y, _ = place()
    return (z + dp * h + dq * (1 - h)) % RING, (y + dp * (1 - h) + dq * h) % RING


def to(h, dp, dq):
    z, y = shifted(h, dp, dq)
    return {"seq": seq_of(z, y, place()[2])}


def across(same_core):
    z, y, core = place()
    target = {"pair": 1 - lax.axis_index("pair")}
    if not same_core:
        target["seq"] = seq_of(z, y, 1 - core)
    return target


def sibling():
    z, y, core = place()
    return {"seq": seq_of(z, y, 1 - core)}


def greet():
    barrier = pltpu.get_barrier_semaphore()
    peers = [to(h, d, 0) for h in range(2) for d in (1, RING - 1)]
    peers += [sibling(), across(True), across(False)]
    for peer in peers:
        pl.semaphore_signal(barrier, inc=1, device_id=peer, device_id_type=MESH)
    pl.semaphore_wait(barrier, len(peers))


def spans(ans_rows, pre_rows):
    pair = lax.axis_index("pair")
    rows = ans_rows + 2 * pre_rows
    half = rows // 2
    parts = (pl.ds(0, half), pl.ds(half, rows - half))
    mine = pl.ds(pl.multiple_of(ans_rows + pair * pre_rows, 16), pre_rows)
    other = pl.ds(pl.multiple_of(ans_rows + (1 - pair) * pre_rows, 16), pre_rows)
    return rows, parts, mine, other


class Copies:
    def __init__(self, send_sem, recv_sem):
        self.send_sem, self.recv_sem = send_sem, recv_sem
        self.ids = {}
        self.sent = []

    def make(self, key, src, dst, to):
        n = self.ids.setdefault(key, len(self.ids))
        return pltpu.make_async_remote_copy(
            src_ref=src,
            dst_ref=dst,
            send_sem=self.send_sem.at[n],
            recv_sem=self.recv_sem.at[n],
            device_id=to,
            device_id_type=MESH,
        )

    def send(self, key, src, dst, to):
        copy = self.make(key, src, dst, to)
        copy.start()
        self.sent.append(copy)

    def arrived(self, key, dst, to):
        self.make(key, dst, dst, to).wait_recv()

    def finish(self):
        for copy in self.sent:
            copy.wait_send()


ORDER = (0, 3, 1, 2)
GATHER_COPIES = 80


def gather_kernel(
    ans_rows,
    pre_rows,
    ak_ref,
    av_ref,
    pk_ref,
    pv_ref,
    q_ref,
    g_ref,
    kv_out,
    q_out,
    g_out,
    held,
    ans_ref,
    pre_ref,
    native,
    split,
    send_sem,
    recv_sem,
    local_sem,
    out_sem,
):
    z, y, core = place()
    rows, parts, mine, other = spans(ans_rows, pre_rows)
    pieces = (pl.ds(0, ans_rows), pl.ds(ans_rows, 2 * pre_rows))
    copies = Copies(send_sem, recv_sem)
    sources = (core, 1 - core)
    stores = []

    def block(r, dp, dq):
        zz, yy = shifted(sources[r], dp, dq)
        return held.at[zz, yy, sources[r]]

    d = HEAD_DIM
    pos = q_ref.shape[1]
    own_rows = pl.ds(pl.multiple_of(core * pos, pos), pos)
    sibling_rows = pl.ds(pl.multiple_of((1 - core) * pos, pos), pos)
    fetches = [pltpu.make_async_copy(ref.at[0], native.at[n], local_sem.at[2 + n]) for n, ref in enumerate((q_ref, g_ref))]
    for copy in fetches:
        copy.start()
    for n, (answer, prefix) in enumerate(((ak_ref, pk_ref), (av_ref, pv_ref))):
        lanes = slice(n * d, (n + 1) * d)
        for c in range(CORES):
            head = slice(c * d, (c + 1) * d)
            ans_ref[c, :, lanes] = jnp.swapaxes(answer[0, :, :, head], 0, 1).reshape(ans_rows, d)
            pre_ref[c, :, lanes] = prefix[:, head]
    greet()
    loads = [
        pltpu.make_async_copy(ans_ref.at[core], block(0, 0, 0).at[pieces[0]], local_sem.at[0]),
        pltpu.make_async_copy(pre_ref.at[core], block(0, 0, 0).at[mine], local_sem.at[1]),
    ]
    for copy in loads:
        copy.start()
    there = held.at[z, y, core]
    copies.send(("sib", 0), ans_ref.at[1 - core], there.at[pieces[0]], sibling())
    copies.send(("sib", 1), pre_ref.at[1 - core], there.at[mine], sibling())
    copies.send(("pair", 0), pre_ref.at[core], there.at[mine], across(True))
    copies.send(("pair", 1), pre_ref.at[1 - core], there.at[mine], across(False))

    def pass_on(key, r, ref, axis, direction):
        target = to(sources[r], direction, 0) if axis == 0 else to(sources[r], 0, direction)
        copies.send(key, ref, ref, target)

    def own(r, piece):
        ref = block(r, 0, 0).at[pieces[piece]]
        source = ans_ref.at[core] if (r, piece) == (0, 0) else ref
        for direction in (1, 3):
            copies.send(("one", r, direction, piece), source, ref, to(sources[r], direction, 0))
        for direction in (1, 3):
            copies.send(("two", r, 0, direction, piece), source, ref, to(sources[r], 0, direction))

    def spread(r, k):
        for direction in (1, 3):
            pass_on(("two", r, k, direction, 2), r, block(r, ORDER[k], 0), 1, direction)

    def keep(r, dp, dq):
        zz, yy = shifted(sources[r], dp, dq)
        store = pltpu.make_async_copy(
            held.at[zz, yy, sources[r]], kv_out.at[zz, yy, sources[r]], out_sem.at[len(stores)]
        )
        store.start()
        stores.append(store)

    own(0, 0)
    copies.arrived(("sib", 0), block(1, 0, 0).at[pieces[0]], sibling())
    own(1, 0)
    loads[0].wait()
    loads[1].wait()
    copies.arrived(("pair", 0), block(0, 0, 0).at[other], across(True))
    own(0, 1)
    keep(0, 0, 0)
    copies.arrived(("sib", 1), block(1, 0, 0).at[mine], sibling())
    copies.arrived(("pair", 1), block(1, 0, 0).at[other], across(False))
    own(1, 1)
    keep(1, 0, 0)
    local_outs = []
    for n, target in enumerate((q_out, g_out)):
        fetches[n].wait()
        features = native.shape[-1] // CORES
        for lane in range(0, native.shape[-1], d):
            c, at = lane // features, lane % features
            split[n, c, :, :, at : at + d] = jnp.swapaxes(native[n, :, :, lane : lane + d], 0, 1)
    for n, target in enumerate((q_out, g_out)):
        copies.send(("sib", 2 + n), split.at[n, 1 - core], target.at[:, own_rows], sibling())
        local_outs.append(pltpu.make_async_copy(split.at[n, core], target.at[:, own_rows], local_sem.at[4 + n]))
        local_outs[n].start()

    for direction in (1, 3):
        for r in range(2):
            back = (-direction) % RING
            for piece in range(2):
                copies.arrived(
                    ("one", r, direction, piece), block(r, back, 0).at[pieces[piece]], to(sources[r], direction, 0)
                )
            n = direction // 2
            pass_on(("far", r, direction), r, block(r, back, 0).at[parts[n]], 0, direction)
            spread(r, ORDER.index(back))
            keep(r, back, 0)
    for r in range(2):
        for direction in (1, 3):
            copies.arrived(
                ("far", r, direction), block(r, 2, 0).at[parts[direction // 2]], to(sources[r], direction, 0)
            )
        spread(r, 3)
        keep(r, 2, 0)
    for k in range(RING):
        for direction in (1, 3):
            for r in range(2):
                back = (-direction) % RING
                here = block(r, ORDER[k], back)
                for piece in range(2) if k == 0 else (2,):
                    area = here if piece == 2 else here.at[pieces[piece]]
                    copies.arrived(("two", r, k, direction, piece), area, to(sources[r], 0, direction))
                pass_on(("far2", r, k, direction), r, here.at[parts[direction // 2]], 1, direction)
                keep(r, ORDER[k], back)
    for k in range(RING):
        for r in range(2):
            here = block(r, ORDER[k], 2)
            for direction in (1, 3):
                copies.arrived(("far2", r, k, direction), here.at[parts[direction // 2]], to(sources[r], 0, direction))
            keep(r, ORDER[k], 2)
    copies.arrived(("sib", 2), q_out.at[:, sibling_rows], sibling())
    copies.arrived(("sib", 3), g_out.at[:, sibling_rows], sibling())
    for store in local_outs + stores:
        store.wait()
    copies.finish()


def gather(answer_keys, answer_values, prefix_keys, prefix_values, queries, grad_out):
    d = HEAD_DIM
    _, pos, batch, features = queries.shape
    ans_rows, pre_rows, width = batch * pos, prefix_keys.shape[0], 2 * d
    rows = ans_rows + 2 * pre_rows
    anywhere = pl.BlockSpec(memory_space=pl.ANY)
    vmem = pl.BlockSpec(memory_space=pltpu.VMEM)
    both = jax.ShapeDtypeStruct((batch, CORES * pos, features // CORES), BF16)
    return pl.pallas_call(
        functools.partial(gather_kernel, ans_rows, pre_rows),
        out_shape=(jax.ShapeDtypeStruct((RING, RING, CORES, rows, width), BF16), both, both),
        in_specs=[vmem] * 4 + [anywhere] * 2,
        out_specs=(anywhere, anywhere, anywhere),
        scratch_shapes=[
            pltpu.VMEM((RING, RING, CORES, rows, width), BF16),
            pltpu.VMEM((CORES, ans_rows, width), BF16),
            pltpu.VMEM((CORES, pre_rows, width), BF16),
            pltpu.VMEM((2, pos, batch, features), BF16),
            pltpu.VMEM((2, CORES, batch, pos, features // CORES), BF16),
            pltpu.SemaphoreType.DMA((GATHER_COPIES,)),
            pltpu.SemaphoreType.DMA((GATHER_COPIES,)),
            pltpu.SemaphoreType.DMA((6,)),
            pltpu.SemaphoreType.DMA((2 * RING * RING,)),
        ],
        compiler_params=pltpu.CompilerParams(collective_id=0, has_side_effects=True),
        name="gather",
    )(answer_keys, answer_values, prefix_keys, prefix_values, queries, grad_out)


SCATTER_COPIES = 60


def scatter_kernel(
    ans_rows,
    pre_rows,
    terms_ref,
    att_ref,
    dq_ref,
    att_final,
    dq_final,
    ak_final,
    av_final,
    pk_final,
    pv_final,
    total,
    split,
    native,
    ans_out,
    pre_out,
    far2,
    near2,
    far1,
    near1,
    ans_swap,
    pre_swap,
    pre_got,
    send_sem,
    recv_sem,
    local_sem,
    out_sem,
):
    z, y, core = place()
    rows, parts, mine, other = spans(ans_rows, pre_rows)
    copies = Copies(send_sem, recv_sem)
    sources = (core, 1 - core)
    order = (2, 1, 3, 0)
    q_order = (2, 1, 3, 0)

    def block(r, dp, dq):
        zz, yy = shifted(sources[r], dp, dq)
        return total.at[zz, yy, sources[r]]

    loads = {}
    for k in range(RING):
        for m in range(1, RING):
            for r in range(2):
                zz, yy = shifted(sources[r], order[k], q_order[m])
                spot = (zz, yy, sources[r])
                n = len(loads)
                loads[r, k, m] = pltpu.make_async_copy(terms_ref.at[spot], total.at[spot], local_sem.at[n])
    pos = att_ref.shape[1] // CORES
    own_rows = pl.ds(pl.multiple_of(core * pos, pos), pos)
    sibling_rows = pl.ds(pl.multiple_of((1 - core) * pos, pos), pos)

    def load(k):
        for m in range(1, RING):
            for r in range(2):
                loads[r, k, m].start()

    def far(k):
        for r in range(2):
            zz, yy = shifted(sources[r], order[k], 2)
            for n, direction in enumerate((1, 3)):
                copies.send(
                    ("far2", r, k, n),
                    terms_ref.at[zz, yy, sources[r], parts[n]],
                    far2.at[r, k, n],
                    to(sources[r], 0, direction),
                )

    def add(into, other_ref):
        into[...] = (into[...].astype(F32) + other_ref[...].astype(F32)).astype(BF16)

    def near(k):
        for r in range(2):
            for n, direction in enumerate((1, 3)):
                loads[r, k, 1 + n].wait()
                here = block(r, order[k], direction)
                copies.arrived(("far2", r, k, n), far2.at[r, k, n], to(sources[r], 0, direction))
                add(here.at[parts[n]], far2.at[r, k, n])
                copies.send(("near2", r, k, n), here, near2.at[r, k, n], to(sources[r], 0, direction))

    def settle2(r, k):
        loads[r, k, 3].wait()
        for n, direction in enumerate((1, 3)):
            copies.arrived(("near2", r, k, n), near2.at[r, k, n], to(sources[r], 0, direction))
        into = block(r, order[k], 0)
        into[...] = (
            into[...].astype(F32) + near2[r, k, 0].astype(F32) + near2[r, k, 1].astype(F32)
        ).astype(BF16)

    load(0)
    greet()
    for k in (0, 1, 2):
        far(k)
    for k in (1, 2, 3):
        load(k)
    outs = []
    for n, ref in enumerate((att_ref, dq_ref)):
        outs.append(pltpu.make_async_copy(ref.at[:, own_rows], split.at[n, core], out_sem.at[n]))
        outs[n].start()
        copies.send(("sib", n), ref.at[:, sibling_rows], split.at[n, core], sibling())
    near(0)
    far(3)
    near(1)
    near(2)
    for r in range(2):
        settle2(r, 0)
        for n, direction in enumerate((1, 3)):
            copies.send(("far1", r, n), block(r, 2, 0).at[parts[n]], far1.at[r, n], to(sources[r], direction, 0))
    near(3)
    d = HEAD_DIM
    finals = []
    for n, target in enumerate((att_final, dq_final)):
        outs[n].wait()
        copies.arrived(("sib", n), split.at[n, 1 - core], sibling())
        features = split.shape[-1]
        for lane in range(0, CORES * features, d):
            c, at = lane // features, lane % features
            native[n, :, :, lane : lane + d] = jnp.swapaxes(split[n, c, :, :, at : at + d], 0, 1)
        finals.append(pltpu.make_async_copy(native.at[n], target.at[0], out_sem.at[2 + n]))
        finals[n].start()
    for k in (1, 2):
        n = k - 1
        direction = order[k]
        for r in range(2):
            settle2(r, k)
            here = block(r, direction, 0)
            copies.arrived(("far1", r, n), far1.at[r, n], to(sources[r], direction, 0))
            add(here.at[parts[n]], far1.at[r, n])
            copies.send(("near1", r, n), here, near1.at[r, n], to(sources[r], direction, 0))
    for r in range(2):
        settle2(r, 3)
    for r in (1, 0):
        for n, direction in enumerate((1, 3)):
            copies.arrived(("near1", r, n), near1.at[r, n], to(sources[r], direction, 0))
        here = block(r, 0, 0)

        def final(area):
            return (
                here[area].astype(F32) + near1[r, 0, area].astype(F32) + near1[r, 1, area].astype(F32)
            )

        pre_swap[r, 0] = final(other).astype(BF16)
        if r == 1:
            copies.send(("pre", 1, 0), pre_swap.at[1, 0], pre_got.at[1, 0], across(False))
            pre_swap[1, 1] = final(mine).astype(BF16)
            copies.send(("pre", 1, 1), pre_swap.at[1, 1], pre_got.at[1, 1], sibling())
            ans_swap[...] = final(pl.ds(0, ans_rows)).astype(BF16)
            copies.send(("ans",), ans_swap, ans_out.at[core], sibling())
        else:
            copies.send(("pre", 0, 0), pre_swap.at[0, 0], pre_got.at[0, 0], across(True))
            pre_out[core] = final(mine)
            ans_out[core] = final(pl.ds(0, ans_rows)).astype(BF16)
    copies.arrived(("pre", 1, 1), pre_got.at[1, 1], sibling())
    copies.arrived(("pre", 1, 0), pre_got.at[1, 0], across(False))
    pre_out[1 - core] = pre_got[1, 0].astype(F32) + pre_got[1, 1].astype(F32)
    copies.arrived(("pre", 0, 0), pre_got.at[0, 0], across(True))
    pre_out[core] = pre_out[core] + pre_got[0, 0].astype(F32)
    copies.arrived(("ans",), ans_out.at[1 - core], sibling())
    for n, (answer, prefix) in enumerate(((ak_final, pk_final), (av_final, pv_final))):
        lanes = slice(n * d, (n + 1) * d)
        for c in range(CORES):
            head = slice(c * d, (c + 1) * d)
            prefix[:, head] = pre_out[c, :, lanes]
            answer[0, :, :, head] = jnp.swapaxes(ans_out[c, :, lanes].reshape(-1, pos, d), 0, 1)
    for copy in finals:
        copy.wait()
    copies.finish()


def scatter(terms, attended, grad_queries, pre_rows):
    rows, width = terms.shape[-2:]
    half = rows // 2
    batch, pos2, features = attended.shape
    pos, ans_rows = pos2 // CORES, rows - 2 * pre_rows
    vmem = pl.BlockSpec(memory_space=pltpu.VMEM)
    anywhere = pl.BlockSpec(memory_space=pl.ANY)
    tokens = jax.ShapeDtypeStruct((1, pos, batch, CORES * features), BF16)
    answers = jax.ShapeDtypeStruct((1, pos, batch, CORES * HEAD_DIM), BF16)
    prefix = jax.ShapeDtypeStruct((pre_rows, CORES * HEAD_DIM), F32)
    return pl.pallas_call(
        functools.partial(scatter_kernel, ans_rows, pre_rows),
        out_shape=(tokens, tokens, answers, answers, prefix, prefix),
        in_specs=[anywhere, anywhere, anywhere],
        out_specs=(anywhere, anywhere, vmem, vmem, vmem, vmem),
        scratch_shapes=[
            pltpu.VMEM((RING, RING, CORES, rows, width), BF16),
            pltpu.VMEM((2, CORES, batch, pos, features), BF16),
            pltpu.VMEM((2, pos, batch, CORES * features), BF16),
            pltpu.VMEM((CORES, ans_rows, width), BF16),
            pltpu.VMEM((CORES, pre_rows, width), F32),
            pltpu.VMEM((CORES, RING, 2, half, width), BF16),
            pltpu.VMEM((CORES, RING, 2, rows, width), BF16),
            pltpu.VMEM((CORES, 2, half, width), BF16),
            pltpu.VMEM((CORES, 2, rows, width), BF16),
            pltpu.VMEM((ans_rows, width), BF16),
            pltpu.VMEM((2, 2, pre_rows, width), BF16),
            pltpu.VMEM((2, 2, pre_rows, width), BF16),
            pltpu.SemaphoreType.DMA((SCATTER_COPIES,)),
            pltpu.SemaphoreType.DMA((SCATTER_COPIES,)),
            pltpu.SemaphoreType.DMA((2 * RING * RING,)),
            pltpu.SemaphoreType.DMA((4,)),
        ],
        compiler_params=pltpu.CompilerParams(collective_id=1, has_side_effects=True),
        name="scatter",
    )(terms, attended, grad_queries)


def nn(a, b):
    return lax.dot_general(a, b, (((1,), (0,)), ((), ())), preferred_element_type=F32)


def nt(a, b):
    return lax.dot_general(a, b, (((1,), (1,)), ((), ())), preferred_element_type=F32)


ANS_SOURCES = 4
PRE_SOURCES = 8


def attend_kernel(
    ans_here,
    pre_rows,
    group,
    length_ref,
    limit_ref,
    q_ref,
    g_ref,
    kv_ref,
    out_ref,
    dq_ref,
    terms_ref,
    scores,
    weights,
    queries,
    douts,
    queries_t,
    douts_t,
    prefix_terms,
    top,
    row_sum,
    acc_t,
):
    sources = kv_ref.shape[0]
    d = HEAD_DIM
    b = pl.program_id(0)
    s = lax.axis_index("seq")
    scale = d**-0.5
    here_rows = CORES * ans_here
    rows = group * here_rows
    ans_chunk = ANS_SOURCES * ans_here
    pre_chunk = PRE_SOURCES * pre_rows
    per_pair = sources // PRE_SOURCES
    pre_total = 2 * sources * pre_rows
    first_row = (s // CORES) * here_rows
    length = length_ref[0, b]
    limit = limit_ref[0, b]
    ans_at = pl.multiple_of(b * ans_here, ans_here)
    live_here = first_row < length
    n_pre = jnp.where(live_here, (limit + pre_chunk - 1) // pre_chunk, 0)
    n_full = jnp.where(live_here, limit // pre_chunk, 0)
    n_ans = jnp.where(live_here, (s // CORES) * CORES // ANS_SOURCES + 1, 0)

    @pl.when(b == 0)
    def _():
        prefix_terms[...] = jnp.zeros_like(prefix_terms)

    terms_ref[:, pl.ds(ans_at, ans_here), :] = jnp.zeros((sources, ans_here, 2 * d), BF16)

    def pre_block(i, lanes):
        pair_at, source = i // per_pair, (i % per_pair) * PRE_SOURCES
        row = pl.multiple_of(2 * ans_here + pair_at * pre_rows, 16)
        part = kv_ref[pl.ds(source, PRE_SOURCES), pl.ds(row, pre_rows), lanes]
        return part.reshape(pre_chunk, d)

    def ans_block(i, lanes):
        part = kv_ref[pl.ds(i * ANS_SOURCES, ANS_SOURCES), pl.ds(ans_at, ans_here), lanes]
        return part.reshape(ans_chunk, d)

    keys_at, values_at = slice(0, d), slice(d, 2 * d)

    def pre_span(i):
        return pl.ds(pl.multiple_of(i * pre_chunk, pre_chunk), pre_chunk)

    def ans_span(i):
        return pl.ds(pl.multiple_of(pre_total + i * ans_chunk, ans_chunk), ans_chunk)

    def fold(values, into):
        return jnp.maximum(into, jnp.max(values.reshape(values.shape[0] // 8, 8, rows), axis=0))

    @pl.when(live_here)
    def _():
        place_rows = lax.broadcasted_iota(jnp.int32, (here_rows, d), 0)
        alive = place_rows + first_row < length
        for g in range(group):
            lanes = slice(g * d, (g + 1) * d)
            here = slice(g * here_rows, (g + 1) * here_rows)
            queries[here] = q_ref[0, :, lanes]
            douts[here] = jnp.where(alive, g_ref[0, :, lanes].astype(F32), 0.0)
        douts_t[...] = douts[...].T
        top[...] = jnp.full_like(top, NEGATIVE)

        def score(i, block, span, keep):
            values = nt(block(i, keys_at), queries[...])
            if keep is not None:
                values = jnp.where(keep(i, values.shape), values, NEGATIVE)
            scores[span(i)] = values
            top[...] = fold(values, top[...])

        def pre_keep(i, shape):
            return lax.broadcasted_iota(jnp.int32, shape, 0) + i * pre_chunk < limit

        def ans_keep(i, shape):
            key = lax.broadcasted_iota(jnp.int32, shape, 0) + i * ans_chunk
            row = lax.broadcasted_iota(jnp.int32, shape, 1) % here_rows + first_row
            return key <= row

        @pl.loop(0, n_full)
        def _(i):
            score(i, pre_block, pre_span, None)

        @pl.when(n_full < n_pre)
        def _():
            score(n_full, pre_block, pre_span, pre_keep)

        @pl.loop(0, n_ans - 1)
        def _(i):
            score(i, ans_block, ans_span, None)

        score(n_ans - 1, ans_block, ans_span, ans_keep)

        top_row = jnp.max(top[...], axis=0, keepdims=True)
        shift = top_row * (scale * LOG2E)
        row_sum[...] = jnp.zeros_like(row_sum)
        acc_t[...] = jnp.zeros_like(acc_t)

        def spread(i, block, span):
            e = jnp.exp2(scores[span(i)] * (scale * LOG2E) - shift)
            row_sum[...] += jnp.sum(e.reshape(e.shape[0] // 8, 8, rows), axis=0)
            low = e.astype(BF16)
            weights[span(i)] = low
            acc_t[...] += nn(block(i, values_at).T, low)

        @pl.loop(0, n_pre)
        def _(i):
            spread(i, pre_block, pre_span)

        @pl.loop(0, n_ans)
        def _(i):
            spread(i, ans_block, ans_span)

        inverse = 1.0 / jnp.sum(row_sum[...], axis=0, keepdims=True)
        attended_t = acc_t[...] * inverse
        scaled = (douts_t[...] * inverse).astype(BF16)
        delta = jnp.sum(scaled.astype(F32) * attended_t, axis=0, keepdims=True)
        douts_low_t = scaled
        queries_t[...] = douts_low_t
        douts_low = douts_low_t.astype(F32).T.astype(BF16)
        attended = attended_t.T
        for g in range(group):
            lanes = slice(g * d, (g + 1) * d)
            here = slice(g * here_rows, (g + 1) * here_rows)
            out_ref[0, :, lanes] = jnp.where(alive, attended[here], 0.0).astype(BF16)
        douts[...] = douts_low.astype(F32)
        acc_t[...] = jnp.zeros_like(acc_t)

        def back(i, block, span):
            low = weights[span(i)]
            grad_probs = nn(block(i, values_at), queries_t[...])
            grad_low = (low.astype(F32) * (grad_probs - delta)).astype(BF16)
            value_term = nn(low, douts_low)
            key_term = nn(grad_low, queries[...]) * scale
            acc_t[...] += nn(block(i, keys_at).T, grad_low)
            return key_term, value_term

        @pl.loop(0, n_pre)
        def _(i):
            key_term, value_term = back(i, pre_block, pre_span)
            prefix_terms[pre_span(i), 0:d] += key_term
            prefix_terms[pre_span(i), d : 2 * d] += value_term

        @pl.loop(0, n_ans)
        def _(i):
            key_term, value_term = back(i, ans_block, ans_span)
            at = pl.ds(i * ANS_SOURCES, ANS_SOURCES)
            span = pl.ds(ans_at, ans_here)
            terms_ref[at, span, 0:d] = key_term.astype(BF16).reshape(ANS_SOURCES, ans_here, d)
            terms_ref[at, span, d : 2 * d] = value_term.astype(BF16).reshape(ANS_SOURCES, ans_here, d)

        grad_queries = (acc_t[...] * scale).T
        for g in range(group):
            lanes = slice(g * d, (g + 1) * d)
            here = slice(g * here_rows, (g + 1) * here_rows)
            dq_ref[0, :, lanes] = grad_queries[here].astype(BF16)

    @pl.when(jnp.logical_not(live_here))
    def _():
        out_ref[...] = jnp.zeros_like(out_ref)
        dq_ref[...] = jnp.zeros_like(dq_ref)

    @pl.when(b == 1)
    def _():
        @pl.loop(0, 2 * per_pair)
        def _(i):
            pair_at, source = i // per_pair, (i % per_pair) * PRE_SOURCES
            row = pl.multiple_of(2 * ans_here + pair_at * pre_rows, 16)
            terms_ref[pl.ds(source, PRE_SOURCES), pl.ds(row, pre_rows), :] = (
                prefix_terms[pre_span(i)].astype(BF16).reshape(PRE_SOURCES, pre_rows, 2 * d)
            )


def attend(queries, grad_out, gathered, lengths, limits, ans_here, pre_rows):
    batch, here_rows, features = queries.shape
    sources, rows_all, width = gathered.shape
    d = HEAD_DIM
    group = features // d
    keys_total = sources * ans_here + 2 * sources * pre_rows
    rows = group * here_rows
    query_spec = pl.BlockSpec((1, here_rows, features), lambda b: (b, 0, 0))
    kv_spec = pl.BlockSpec((sources, rows_all, width), lambda b: (0, 0, 0))
    smem = pl.BlockSpec(memory_space=pltpu.SMEM)
    return pl.pallas_call(
        functools.partial(attend_kernel, ans_here, pre_rows, group),
        grid=(batch,),
        out_shape=(
            jax.ShapeDtypeStruct(queries.shape, BF16),
            jax.ShapeDtypeStruct(queries.shape, BF16),
            jax.ShapeDtypeStruct(gathered.shape, BF16),
        ),
        in_specs=[smem, smem, query_spec, query_spec, kv_spec],
        out_specs=(query_spec, query_spec, kv_spec),
        scratch_shapes=[
            pltpu.VMEM((keys_total, rows), F32),
            pltpu.VMEM((keys_total, rows), BF16),
            pltpu.VMEM((rows, d), BF16),
            pltpu.VMEM((rows, d), F32),
            pltpu.VMEM((d, rows), BF16),
            pltpu.VMEM((d, rows), F32),
            pltpu.VMEM((2 * sources * pre_rows, width), F32),
            pltpu.VMEM((8, rows), F32),
            pltpu.VMEM((8, rows), F32),
            pltpu.VMEM((d, rows), F32),
        ],
        compiler_params=pltpu.CompilerParams(
            dimension_semantics=("arbitrary",), vmem_limit_bytes=60 * 1024 * 1024
        ),
        name="attend",
    )(lengths, limits, queries, grad_out, gathered)


def on_device(
    queries,
    answer_keys,
    answer_values,
    prefix_keys,
    prefix_values,
    grad_out,
    answer_length,
    prefix_limit,
):
    ans_here, pre_rows = queries.shape[1], prefix_keys.shape[0]
    gathered, q_here, g_here = gather(
        answer_keys, answer_values, prefix_keys, prefix_values, queries, grad_out
    )
    flat = gathered.reshape((-1,) + gathered.shape[-2:])
    attended, grad_q, terms = attend(q_here, g_here, flat, answer_length, prefix_limit, ans_here, pre_rows)
    return scatter(terms.reshape(gathered.shape), attended, grad_q, pre_rows)


def solution(mesh):
    tokens = P("pair", "seq", None, "head")
    prefix = P(("pair", "seq"), "head")
    scalars = P("pair", None)
    return jax.shard_map(
        on_device,
        mesh=mesh,
        in_specs=(tokens, tokens, tokens, prefix, prefix, tokens, scalars, scalars),
        out_specs=(tokens, tokens, tokens, tokens, prefix, prefix),
        check_vma=False,
    )
```

```python
import functools

import jax
import jax.numpy as jnp
from jax import lax
from jax.experimental import pallas as pl
from jax.experimental.pallas import tpu as pltpu
from jax.sharding import PartitionSpec as P

HEAD_DIM = 128
RING = 4
CORES = 2
LOG2E = 1.4426950408889634
NEGATIVE = -1e30
MESH = pl.DeviceIdType.MESH
BF16 = jnp.bfloat16
F32 = jnp.float32


def place():
    s = lax.axis_index("seq")
    return s // (RING * CORES), (s // CORES) % RING, s % CORES


def seq_of(z, y, core):
    return (z * RING + y) * CORES + core


def shifted(h, dp, dq):
    z, y, _ = place()
    return (z + dp * h + dq * (1 - h)) % RING, (y + dp * (1 - h) + dq * h) % RING


def to(h, dp, dq):
    z, y = shifted(h, dp, dq)
    return {"seq": seq_of(z, y, place()[2])}


def across(same_core):
    z, y, core = place()
    target = {"pair": 1 - lax.axis_index("pair")}
    if not same_core:
        target["seq"] = seq_of(z, y, 1 - core)
    return target


def sibling():
    z, y, core = place()
    return {"seq": seq_of(z, y, 1 - core)}


PEERS = 7


def greet():
    barrier = pltpu.get_barrier_semaphore()
    peers = [to(h, d, 0) for h in range(2) for d in (1, RING - 1)]
    peers += [sibling(), across(True), across(False)]
    for peer in peers:
        pl.semaphore_signal(barrier, inc=1, device_id=peer, device_id_type=MESH)


def met():
    pl.semaphore_wait(pltpu.get_barrier_semaphore(), PEERS)


def spans(ans_rows, pre_rows):
    pair = lax.axis_index("pair")
    rows = ans_rows + 2 * pre_rows
    half = rows // 2
    parts = (pl.ds(0, half), pl.ds(half, rows - half))
    mine = pl.ds(pl.multiple_of(ans_rows + pair * pre_rows, 16), pre_rows)
    other = pl.ds(pl.multiple_of(ans_rows + (1 - pair) * pre_rows, 16), pre_rows)
    return rows, parts, mine, other


class Copies:
    def __init__(self, send_sem, recv_sem):
        self.send_sem, self.recv_sem = send_sem, recv_sem
        self.ids = {}
        self.sent = []

    def make(self, key, src, dst, to):
        n = self.ids.setdefault(key, len(self.ids))
        return pltpu.make_async_remote_copy(
            src_ref=src,
            dst_ref=dst,
            send_sem=self.send_sem.at[n],
            recv_sem=self.recv_sem.at[n],
            device_id=to,
            device_id_type=MESH,
        )

    def send(self, key, ends):
        self.make(key, *ends()).start()
        self.sent.append((key, ends))

    def arrived(self, key, dst, to):
        self.make(key, dst, dst, to).wait_recv()

    def finish(self):
        for key, ends in self.sent:
            self.make(key, *ends()).wait_send()


def pick(i, values):
    chosen = jnp.int32(values[0])
    for n in range(1, len(values)):
        chosen = jnp.where(i == n, jnp.int32(values[n]), chosen)
    return chosen


def run_at(condition, step):
    @pl.when(condition)
    def _():
        step()


def nn(a, b):
    return lax.dot_general(a, b, (((1,), (0,)), ((), ())), preferred_element_type=F32)


def nt(a, b):
    return lax.dot_general(a, b, (((1,), (1,)), ((), ())), preferred_element_type=F32)


COPIES = 104
ORDER = (0, 3, 1, 2)
FORWARD = (
    (0, 0), (3, 0), (1, 0), (0, 3), (0, 1), (2, 0), (3, 3), (3, 1),
    (1, 3), (1, 1), (0, 2), (2, 3), (2, 1), (3, 2), (1, 2), (2, 2),
)
BACK_P = (2, 1, 3, 0)
BACKWARD = (
    (0, 2), (1, 2), (0, 1), (0, 3), (2, 2), (1, 1), (1, 3), (0, 0),
    (3, 2), (2, 1), (2, 3), (1, 0), (3, 1), (3, 3), (2, 0), (3, 0),
)


def layer_kernel(
    group,
    length_ref,
    limit_ref,
    ak_ref,
    av_ref,
    pk_ref,
    pv_ref,
    q_ref,
    g_ref,
    att_final,
    dq_final,
    ak_final,
    av_final,
    pk_final,
    pv_final,
    held,
    total,
    staged_ans,
    staged_pre,
    answers_in,
    prefix_in,
    native,
    split,
    rows_ref,
    weights,
    tops,
    top_now,
    row_sum,
    acc_t,
    douts,
    douts_t,
    delta_ref,
    masked_queries,
    probs_low,
    fin,
    ans_out,
    pre_out,
    far2,
    near2,
    far1,
    near1,
    ans_swap,
    pre_swap,
    pre_got,
    send_sem,
    recv_sem,
    local_sem,
):
    d = HEAD_DIM
    z, y, core = place()
    pos = q_ref.shape[1]
    batch = q_ref.shape[2]
    ans_rows = batch * pos
    pre_rows = pk_ref.shape[0]
    sources_total = RING * RING * CORES
    here_rows = CORES * pos
    rows = group * here_rows
    scale = d**-0.5
    factor = scale * LOG2E
    chip = z * RING + y
    pair = lax.axis_index("pair")
    block_rows, parts, mine, other = spans(ans_rows, pre_rows)
    pieces = (pl.ds(0, ans_rows), pl.ds(ans_rows, 2 * pre_rows))
    copies = Copies(send_sem, recv_sem)
    sources = (core, 1 - core)

    def held_at(r, dp, dq):
        zz, yy = shifted(sources[r], dp, dq)
        return held.at[zz, yy, sources[r]]

    def total_at(r, dp, dq):
        zz, yy = shifted(sources[r], dp, dq)
        return total.at[zz, yy, sources[r]]

    greet()
    small_fetches = [
        pltpu.make_async_copy(ref, small, local_sem.at[6 + n])
        for n, (ref, small) in enumerate(
            zip((ak_ref, av_ref, pk_ref, pv_ref), (answers_in.at[0], answers_in.at[1], prefix_in.at[0], prefix_in.at[1]))
        )
    ]

    def fetch(n):
        return pltpu.make_async_copy((q_ref, g_ref)[n].at[0], native.at[n], local_sem.at[n])

    for copy in small_fetches + [fetch(0), fetch(1)]:
        copy.start()
    for copy in small_fetches:
        copy.wait()
    for n in range(2):
        lanes = slice(n * d, (n + 1) * d)
        for c in range(CORES):
            head = slice(c * d, (c + 1) * d)
            staged_ans[c, :, lanes] = jnp.swapaxes(answers_in[n, 0, :, :, head], 0, 1).reshape(ans_rows, d)
            staged_pre[c, :, lanes] = prefix_in[n, :, head]
    met()
    loads = [
        pltpu.make_async_copy(staged_ans.at[core], held.at[z, y, core, pieces[0]], local_sem.at[2]),
        pltpu.make_async_copy(staged_pre.at[core], held.at[z, y, core, mine], local_sem.at[3]),
    ]
    for copy in loads:
        copy.start()
    there = held.at[z, y, core]
    copies.send(("sib", 0), lambda: (staged_ans.at[1 - core], there.at[pieces[0]], sibling()))
    copies.send(("sib", 1), lambda: (staged_pre.at[1 - core], there.at[mine], sibling()))
    copies.send(("pair", 0), lambda: (staged_pre.at[core], there.at[mine], across(True)))
    copies.send(("pair", 1), lambda: (staged_pre.at[1 - core], there.at[mine], across(False)))

    def own(r, piece):
        ref = held_at(r, 0, 0).at[pieces[piece]]
        source = staged_ans.at[core] if (r, piece) == (0, 0) else ref
        for direction in (1, 3):
            copies.send(
                ("one", r, direction, piece), lambda direction=direction: (source, ref, to(sources[r], direction, 0))
            )
        for direction in (1, 3):
            copies.send(
                ("two", r, 0, direction, piece), lambda direction=direction: (source, ref, to(sources[r], 0, direction))
            )

    def spread(k):
        for r in range(2):
            for direction in (1, 3):

                def ends(r=r, direction=direction):
                    ref = held_at(r, ORDER[k], 0)
                    return ref, ref, to(sources[r], 0, direction)

                copies.send(("two", r, k, direction, 2), ends)

    def head_lanes(c, g):
        return pl.ds(pl.multiple_of((c * group + g) * d, d), d)

    def lay_out(n):
        fetch(n).wait()
        for g in range(group):
            split[n, :, g] = jnp.swapaxes(native[n, :, :, head_lanes(1 - core, g)], 0, 1)
        copies.send(("q", n), lambda: (split.at[n], rows_ref.at[n, :, :, core], sibling()))
        for g in range(group):
            rows_ref[n, :, g, core] = jnp.swapaxes(native[n, :, :, head_lanes(core, g)], 0, 1)

    def laid_out(n):
        copies.arrived(("q", n), rows_ref.at[n, :, :, 1 - core], sibling())

    own(0, 0)
    lay_out(0)
    copies.arrived(("sib", 0), held_at(1, 0, 0).at[pieces[0]], sibling())
    own(1, 0)
    for copy in loads:
        copy.wait()
    copies.arrived(("pair", 0), held_at(0, 0, 0).at[other], across(True))
    own(0, 1)
    copies.arrived(("sib", 1), held_at(1, 0, 0).at[mine], sibling())
    copies.arrived(("pair", 1), held_at(1, 0, 0).at[other], across(False))
    own(1, 1)
    laid_out(0)

    def first_neighbours():
        for direction in (1, 3):
            back = (-direction) % RING
            for r in range(2):
                for piece in range(2):
                    copies.arrived(
                        ("one", r, direction, piece),
                        held_at(r, back, 0).at[pieces[piece]],
                        to(sources[r], direction, 0),
                    )

                def ends(r=r, direction=direction, back=back):
                    ref = held_at(r, back, 0).at[parts[direction // 2]]
                    return ref, ref, to(sources[r], direction, 0)

                copies.send(("far", r, direction), ends)
            spread(ORDER.index(back))

    def first_far():
        for r in range(2):
            for direction in (1, 3):
                copies.arrived(
                    ("far", r, direction), held_at(r, 2, 0).at[parts[direction // 2]], to(sources[r], direction, 0)
                )
        spread(3)

    def second_neighbours(k):
        for direction in (1, 3):
            back = (-direction) % RING
            for r in range(2):
                here = held_at(r, ORDER[k], back)
                for piece in range(2) if k == 0 else (2,):
                    area = here if piece == 2 else here.at[pieces[piece]]
                    copies.arrived(("two", r, k, direction, piece), area, to(sources[r], 0, direction))

                def ends(r=r, direction=direction, back=back):
                    ref = held_at(r, ORDER[k], back).at[parts[direction // 2]]
                    return ref, ref, to(sources[r], 0, direction)

                copies.send(("far2", r, k, direction), ends)

    def second_far(k):
        for r in range(2):
            here = held_at(r, ORDER[k], 2)
            for direction in (1, 3):
                copies.arrived(("far2", r, k, direction), here.at[parts[direction // 2]], to(sources[r], 0, direction))

    forward_steps = {
        1: first_neighbours,
        2: lambda: lay_out(1),
        3: lambda: second_neighbours(0),
        5: first_far,
        6: lambda: second_neighbours(1),
        8: lambda: second_neighbours(2),
        10: lambda: second_far(0),
        11: lambda: second_neighbours(3),
        13: lambda: second_far(1),
        14: lambda: second_far(2),
        15: lambda: second_far(3),
    }
    top_now[...] = jnp.full_like(top_now, NEGATIVE)
    row_sum[...] = jnp.zeros_like(row_sum)
    acc_t[...] = jnp.zeros_like(acc_t)

    def cat(b, dp, dq, lanes):
        spots = [held_at(r, dp, dq) for r in range(2)]
        return jnp.concatenate(
            [spot[b * pos : (b + 1) * pos, lanes] for spot in spots] + [spot[ans_rows:block_rows, lanes] for spot in spots],
            axis=0,
        )

    keys_at, values_at = slice(0, d), slice(d, 2 * d)

    def mask_features(b, dp, dq):
        limit = limit_ref[0, b]

        def one_hot(feature):
            lane = lax.broadcasted_iota(jnp.int32, feature.shape, 1)
            return jnp.where(lane == feature, 1.0, 0.0)

        ans_part, pre_part = [], []
        for r in range(2):
            zz, yy = shifted(sources[r], dp, dq)
            source = (zz * RING + yy) * CORES + sources[r]
            key = lax.broadcasted_iota(jnp.int32, (pos, d), 0) + (source * pos - chip * here_rows)
            ans_part.append(one_hot(jnp.where(key <= 0, -1, jnp.where(key < here_rows, key, 0))))
            for p in range(2):
                token = lax.broadcasted_iota(jnp.int32, (pre_rows, d), 0) + (p * sources_total + source) * pre_rows
                pre_part.append(one_hot(jnp.where(token < limit, -1, 0)))
        return jnp.concatenate(ans_part + pre_part, axis=0).astype(BF16)

    def query_rows(n, b):
        return rows_ref[n, b].reshape(rows, d)

    tiles = [slice(lo, min(lo + 2 * d, rows)) for lo in range(0, rows, 2 * d)]
    mask_row = lax.broadcasted_iota(jnp.int32, (here_rows, d), 0)
    mask_lane = lax.broadcasted_iota(jnp.int32, (here_rows, d), 1)
    row_mask = jnp.where((mask_lane == 0) | (mask_lane > mask_row), NEGATIVE, 0.0).astype(BF16)
    for b in range(batch):
        masked_queries[b, :, 0:d] = query_rows(0, b)
        for g in range(group):
            masked_queries[b, g * here_rows : (g + 1) * here_rows, d : 2 * d] = row_mask

    @pl.loop(0, RING * RING)
    def _(i):
        for n, step in forward_steps.items():
            run_at(i == n, step)
        dp = pick(i, [f[0] for f in FORWARD])
        dq = pick(i, [f[1] for f in FORWARD])
        at = dp * RING + dq
        def softmax(b, span, scores):
            before = top_now[b, :, span]
            folded = jnp.max(scores.reshape(-1, 8, scores.shape[1]), axis=0)
            now = jnp.maximum(before, jnp.max(folded, axis=0, keepdims=True))
            top_now[b, :, span] = now
            tops[b, at, :, span] = now
            ratio = jnp.exp2((before - now) * factor)
            e = jnp.exp2(scores * factor - now[0:1] * factor)
            row_sum[b, :, span] = row_sum[b, :, span] * ratio + jnp.sum(e.reshape(-1, 8, e.shape[1]), axis=0)
            low = e.astype(BF16)
            weights[b, at, :, span] = low
            return ratio, low

        keys = [
            jnp.concatenate([cat(b, dp, dq, keys_at), mask_features(b, dp, dq)], axis=1) for b in range(batch)
        ]
        values_t = [cat(b, dp, dq, values_at).T for b in range(batch)]

        scores = [[nt(keys[b], masked_queries[b, span]) for span in tiles] for b in range(batch)]
        for b in range(batch):
            ratios = []
            for span, tile in zip(tiles, scores[b]):
                ratios.append(softmax(b, span, tile)[0][0:1])
            acc_t[b] = acc_t[b] * jnp.concatenate(ratios, axis=1) + nn(values_t[b], weights[b, at])

    laid_out(1)
    for b in range(batch):
        inverse = 1.0 / jnp.sum(row_sum[b], axis=0, keepdims=True)
        attended_t = acc_t[b] * inverse
        alive = lax.broadcasted_iota(jnp.int32, (here_rows, d), 0) + chip * here_rows < length_ref[0, b]
        alive = jnp.concatenate([jnp.where(alive, 1.0, 0.0)] * group, axis=0)
        live_grad = jnp.where(alive > 0.5, query_rows(1, b).astype(F32), 0.0)
        scaled_t = (live_grad.T * inverse).astype(BF16)
        delta_ref[b] = jnp.broadcast_to(
            jnp.sum(scaled_t.astype(F32) * attended_t, axis=0, keepdims=True), delta_ref.shape[1:]
        )
        douts_t[b] = scaled_t
        douts[b] = scaled_t.astype(F32).T.astype(BF16)
        attended = jnp.where(alive > 0.5, attended_t.T, 0.0).astype(BF16)
        rows_ref[1, b] = attended.reshape(rows_ref.shape[2:])
        acc_t[b] = jnp.zeros_like(acc_t[b])

    def away(n, target):
        return pltpu.make_async_copy(native.at[n], target.at[0], local_sem.at[4 + n])

    def leave(n):
        copies.send(("out", n), lambda: (rows_ref.at[1 - n, :, :, 1 - core], fin.at[n], sibling()))
        for g in range(group):
            native[n, :, :, head_lanes(core, g)] = jnp.swapaxes(rows_ref[1 - n, :, g, core], 0, 1)

    def settle_rows(n, target):
        copies.arrived(("out", n), fin.at[n], sibling())
        for g in range(group):
            native[n, :, :, head_lanes(1 - core, g)] = jnp.swapaxes(fin[n, :, g], 0, 1)
        away(n, target).start()

    leave(0)

    def add(into, other_ref):
        into[...] = (into[...].astype(F32) + other_ref[...].astype(F32)).astype(BF16)

    def far(k):
        for r in range(2):
            for n, direction in enumerate((1, 3)):

                def ends(r=r, n=n, direction=direction):
                    ref = total_at(r, BACK_P[k], 2).at[parts[n]]
                    return ref, far2.at[r, k, n], to(sources[r], 0, direction)

                copies.send(("back far2", r, k, n), ends)

    def near(k):
        for r in range(2):
            for n, direction in enumerate((1, 3)):
                copies.arrived(("back far2", r, k, n), far2.at[r, k, n], to(sources[r], 0, direction))
                add(total_at(r, BACK_P[k], direction).at[parts[n]], far2.at[r, k, n])

                def ends(r=r, n=n, direction=direction):
                    return total_at(r, BACK_P[k], direction), near2.at[r, k, n], to(sources[r], 0, direction)

                copies.send(("back near2", r, k, n), ends)

    def settle(k):
        for r in range(2):
            for n, direction in enumerate((1, 3)):
                copies.arrived(("back near2", r, k, n), near2.at[r, k, n], to(sources[r], 0, direction))
            into = total_at(r, BACK_P[k], 0)
            into[...] = (
                into[...].astype(F32) + near2[r, k, 0].astype(F32) + near2[r, k, 1].astype(F32)
            ).astype(BF16)

    def far_first():
        for r in range(2):
            for n, direction in enumerate((1, 3)):

                def ends(r=r, n=n, direction=direction):
                    return total_at(r, 2, 0).at[parts[n]], far1.at[r, n], to(sources[r], direction, 0)

                copies.send(("back far1", r, n), ends)

    def near_first(k):
        n, direction = k - 1, BACK_P[k]
        for r in range(2):
            copies.arrived(("back far1", r, n), far1.at[r, n], to(sources[r], direction, 0))
            add(total_at(r, direction, 0).at[parts[n]], far1.at[r, n])

            def ends(r=r):
                return total_at(r, direction, 0), near1.at[r, n], to(sources[r], direction, 0)

            copies.send(("back near1", r, n), ends)

    back_steps = {
        0: lambda: far(0),
        1: lambda: (far(1), settle_rows(0, att_final)),
        3: lambda: near(0),
        4: lambda: far(2),
        6: lambda: near(1),
        8: lambda: (far(3), settle(0), far_first()),
        10: lambda: near(2),
        11: lambda: (settle(1), near_first(1)),
        13: lambda: near(3),
        14: lambda: (settle(2), near_first(2)),
    }

    @pl.loop(0, RING * RING)
    def _(j):
        dp = pick(j, [BACK_P[f[0]] for f in BACKWARD])
        dq = pick(j, [f[1] for f in BACKWARD])
        at = dp * RING + dq
        key_terms, value_terms = [], []
        for b in range(batch):
            values = cat(b, dp, dq, values_at)
            for span in tiles:
                ratio = jnp.exp2((tops[b, at, :, span] - top_now[b, :, span]) * factor)[0:1]
                low = (weights[b, at, :, span].astype(F32) * ratio).astype(BF16)
                probs_low[b, :, span] = low
                grad_probs = nn(values, douts_t[b, :, span])
                grad_low = low.astype(F32) * (grad_probs - delta_ref[b, 0:1, span])
                weights[b, at, :, span] = grad_low.astype(BF16)
            value_terms.append(nn(probs_low[b], douts[b]))
            key_terms.append(nn(weights[b, at], query_rows(0, b)) * scale)
        for lanes, terms in ((keys_at, key_terms), (values_at, value_terms)):
            prefix = sum(terms)[CORES * pos :]
            for r in range(2):
                spot = total_at(r, dp, dq)
                for b in range(batch):
                    spot[b * pos : (b + 1) * pos, lanes] = terms[b][r * pos : (r + 1) * pos].astype(BF16)
                spot[ans_rows:block_rows, lanes] = prefix[r * 2 * pre_rows : (r + 1) * 2 * pre_rows].astype(BF16)
        for n, step in back_steps.items():
            run_at(j == n, step)

    @pl.loop(0, RING)
    def _(dp):
        for b in range(batch):
            keys = jnp.concatenate([cat(b, dp, dq, keys_at).T for dq in range(RING)], axis=1)
            grads = weights[b, pl.ds(dp * RING, RING)]
            acc_t[b] += nn(keys, grads.reshape(-1, rows))

    for b in range(batch):
        rows_ref[0, b] = (acc_t[b] * scale).T.astype(BF16).reshape(rows_ref.shape[2:])
    leave(1)
    settle(3)
    for r in (1, 0):
        for n, direction in enumerate((1, 3)):
            copies.arrived(("back near1", r, n), near1.at[r, n], to(sources[r], direction, 0))
        here = total_at(r, 0, 0)

        def final(area):
            return here[area].astype(F32) + near1[r, 0, area].astype(F32) + near1[r, 1, area].astype(F32)

        pre_swap[r, 0] = final(other).astype(BF16)
        if r == 1:
            copies.send(("pre", 1, 0), lambda: (pre_swap.at[1, 0], pre_got.at[1, 0], across(False)))
            pre_swap[1, 1] = final(mine).astype(BF16)
            copies.send(("pre", 1, 1), lambda: (pre_swap.at[1, 1], pre_got.at[1, 1], sibling()))
            ans_swap[...] = final(pl.ds(0, ans_rows)).astype(BF16)
            copies.send(("ans",), lambda: (ans_swap, ans_out.at[core], sibling()))
        else:
            copies.send(("pre", 0, 0), lambda: (pre_swap.at[0, 0], pre_got.at[0, 0], across(True)))
            pre_out[core] = final(mine)
            ans_out[core] = final(pl.ds(0, ans_rows)).astype(BF16)
    settle_rows(1, dq_final)
    copies.arrived(("pre", 1, 1), pre_got.at[1, 1], sibling())
    copies.arrived(("pre", 1, 0), pre_got.at[1, 0], across(False))
    pre_out[1 - core] = pre_got[1, 0].astype(F32) + pre_got[1, 1].astype(F32)
    copies.arrived(("pre", 0, 0), pre_got.at[0, 0], across(True))
    pre_out[core] = pre_out[core] + pre_got[0, 0].astype(F32)
    copies.arrived(("ans",), ans_out.at[1 - core], sibling())
    for n, (answer, prefix) in enumerate(((ak_final, pk_final), (av_final, pv_final))):
        lanes = slice(n * d, (n + 1) * d)
        for c in range(CORES):
            head = slice(c * d, (c + 1) * d)
            prefix[:, head] = pre_out[c, :, lanes]
            answer[0, :, :, head] = jnp.swapaxes(ans_out[c, :, lanes].reshape(-1, pos, d), 0, 1)
    away(0, att_final).wait()
    away(1, dq_final).wait()
    copies.finish()


def layer(lengths, limits, answer_keys, answer_values, prefix_keys, prefix_values, queries, grad_out):
    d = HEAD_DIM
    _, pos, batch, features = queries.shape
    group = features // d // CORES
    rows, width = group * CORES * pos, 2 * d
    ans_rows, pre_rows = batch * pos, prefix_keys.shape[0]
    block = ans_rows + 2 * pre_rows
    half = block // 2
    groups = RING * RING
    keys = CORES * (pos + 2 * pre_rows)
    vmem = pl.BlockSpec(memory_space=pltpu.VMEM)
    smem = pl.BlockSpec(memory_space=pltpu.SMEM)
    anywhere = pl.BlockSpec(memory_space=pl.ANY)
    tokens = jax.ShapeDtypeStruct(queries.shape, BF16)
    answers = jax.ShapeDtypeStruct(answer_keys.shape, BF16)
    prefix = jax.ShapeDtypeStruct(prefix_keys.shape, F32)
    per_head = (batch, group, pos, d)
    return pl.pallas_call(
        functools.partial(layer_kernel, group),
        out_shape=(tokens, tokens, answers, answers, prefix, prefix),
        in_specs=[smem] * 2 + [anywhere] * 6,
        out_specs=(anywhere, anywhere, vmem, vmem, vmem, vmem),
        scratch_shapes=[
            pltpu.VMEM((RING, RING, CORES, block, width), BF16),
            pltpu.VMEM((RING, RING, CORES, block, width), BF16),
            pltpu.VMEM((CORES, ans_rows, width), BF16),
            pltpu.VMEM((CORES, pre_rows, width), BF16),
            pltpu.VMEM((2,) + answer_keys.shape, BF16),
            pltpu.VMEM((2,) + prefix_keys.shape, BF16),
            pltpu.VMEM((2, pos, batch, features), BF16),
            pltpu.VMEM((2,) + per_head, BF16),
            pltpu.VMEM((2, batch, group, CORES, pos, d), BF16),
            pltpu.VMEM((batch, groups, keys, rows), BF16),
            pltpu.VMEM((batch, groups, 8, rows), F32),
            pltpu.VMEM((batch, 8, rows), F32),
            pltpu.VMEM((batch, 8, rows), F32),
            pltpu.VMEM((batch, d, rows), F32),
            pltpu.VMEM((batch, rows, d), BF16),
            pltpu.VMEM((batch, d, rows), BF16),
            pltpu.VMEM((batch, 8, rows), F32),
            pltpu.VMEM((batch, rows, 2 * d), BF16),
            pltpu.VMEM((batch, keys, rows), BF16),
            pltpu.VMEM((2,) + per_head, BF16),
            pltpu.VMEM((CORES, ans_rows, width), BF16),
            pltpu.VMEM((CORES, pre_rows, width), F32),
            pltpu.VMEM((CORES, RING, 2, half, width), BF16),
            pltpu.VMEM((CORES, RING, 2, block, width), BF16),
            pltpu.VMEM((CORES, 2, half, width), BF16),
            pltpu.VMEM((CORES, 2, block, width), BF16),
            pltpu.VMEM((ans_rows, width), BF16),
            pltpu.VMEM((2, 2, pre_rows, width), BF16),
            pltpu.VMEM((2, 2, pre_rows, width), BF16),
            pltpu.SemaphoreType.DMA((COPIES,)),
            pltpu.SemaphoreType.DMA((COPIES,)),
            pltpu.SemaphoreType.DMA((10,)),
        ],
        compiler_params=pltpu.CompilerParams(
            collective_id=0, has_side_effects=True, vmem_limit_bytes=60 * 1024 * 1024
        ),
        name="layer",
    )(lengths, limits, answer_keys, answer_values, prefix_keys, prefix_values, queries, grad_out)


def settle_kernel(count, *refs):
    ins, outs, held, sems = refs[:count], refs[count : 2 * count], refs[2 * count : 3 * count], refs[3 * count]
    takes = [pltpu.make_async_copy(ins[n], held[n], sems.at[n]) for n in range(count)]
    gives = [pltpu.make_async_copy(held[n], outs[n], sems.at[count + n]) for n in range(count)]
    for copy in takes:
        copy.start()
    for take, give in zip(takes, gives):
        take.wait()
        give.start()
    for copy in gives:
        copy.wait()


def settle_results(results):
    count = len(results)
    anywhere = pl.BlockSpec(memory_space=pl.ANY)
    return pl.pallas_call(
        functools.partial(settle_kernel, count),
        out_shape=tuple(jax.ShapeDtypeStruct(x.shape, x.dtype) for x in results),
        in_specs=[anywhere] * count,
        out_specs=(anywhere,) * count,
        scratch_shapes=[pltpu.VMEM(x.shape, x.dtype) for x in results]
        + [pltpu.SemaphoreType.DMA((2 * count,))],
        name="settle",
    )(*results)


def on_device(
    queries,
    answer_keys,
    answer_values,
    prefix_keys,
    prefix_values,
    grad_out,
    answer_length,
    prefix_limit,
):
    return settle_results(
        layer(
            answer_length,
            prefix_limit,
            answer_keys,
            answer_values,
            prefix_keys,
            prefix_values,
            queries,
            grad_out,
        )
    )


def solution(mesh):
    tokens = P("pair", "seq", None, "head")
    prefix = P(("pair", "seq"), "head")
    scalars = P("pair", None)
    return jax.shard_map(
        on_device,
        mesh=mesh,
        in_specs=(tokens, tokens, tokens, prefix, prefix, tokens, scalars, scalars),
        out_specs=(tokens, tokens, tokens, tokens, prefix, prefix),
        check_vma=False,
    )
```

```python
import functools

import jax
import jax.numpy as jnp
from jax import lax
from jax.experimental import pallas as pl
from jax.experimental.pallas import tpu as pltpu
from jax.sharding import PartitionSpec as P

HEAD_DIM = 128
RING = 4
CORES = 2
LOG2E = 1.4426950408889634
NEGATIVE = -1e30
MESH = pl.DeviceIdType.MESH
BF16 = jnp.bfloat16
F32 = jnp.float32


def place():
    s = lax.axis_index("seq")
    return s // (RING * CORES), (s // CORES) % RING, s % CORES


def seq_of(z, y, core):
    return (z * RING + y) * CORES + core


def shifted(h, dp, dq):
    z, y, _ = place()
    return (z + dp * h + dq * (1 - h)) % RING, (y + dp * (1 - h) + dq * h) % RING


def to(h, dp, dq):
    z, y = shifted(h, dp, dq)
    return {"seq": seq_of(z, y, place()[2])}


def across(same_core):
    z, y, core = place()
    target = {"pair": 1 - lax.axis_index("pair")}
    if not same_core:
        target["seq"] = seq_of(z, y, 1 - core)
    return target


def sibling():
    z, y, core = place()
    return {"seq": seq_of(z, y, 1 - core)}


PEERS = 7


def greet():
    barrier = pltpu.get_barrier_semaphore()
    peers = [to(h, d, 0) for h in range(2) for d in (1, RING - 1)]
    peers += [sibling(), across(True), across(False)]
    for peer in peers:
        pl.semaphore_signal(barrier, inc=1, device_id=peer, device_id_type=MESH)


def met():
    pl.semaphore_wait(pltpu.get_barrier_semaphore(), PEERS)


def spans(ans_rows, pre_rows):
    pair = lax.axis_index("pair")
    rows = ans_rows + 2 * pre_rows
    half = rows // 2
    parts = (pl.ds(0, half), pl.ds(half, rows - half))
    mine = pl.ds(pl.multiple_of(ans_rows + pair * pre_rows, 16), pre_rows)
    other = pl.ds(pl.multiple_of(ans_rows + (1 - pair) * pre_rows, 16), pre_rows)
    return rows, parts, mine, other


class Copies:
    def __init__(self, send_sem, recv_sem):
        self.send_sem, self.recv_sem = send_sem, recv_sem
        self.ids = {}
        self.sent = []

    def make(self, key, src, dst, to):
        n = self.ids.setdefault(key, len(self.ids))
        return pltpu.make_async_remote_copy(
            src_ref=src,
            dst_ref=dst,
            send_sem=self.send_sem.at[n],
            recv_sem=self.recv_sem.at[n],
            device_id=to,
            device_id_type=MESH,
        )

    def send(self, key, ends):
        self.make(key, *ends()).start()
        self.sent.append((key, ends))

    def arrived(self, key, dst, to):
        self.make(key, dst, dst, to).wait_recv()

    def finish(self):
        for key, ends in self.sent:
            self.make(key, *ends()).wait_send()


def pick(i, values):
    chosen = jnp.int32(values[0])
    for n in range(1, len(values)):
        chosen = jnp.where(i == n, jnp.int32(values[n]), chosen)
    return chosen


def run_at(condition, step):
    @pl.when(condition)
    def _():
        step()


def nn(a, b):
    return lax.dot_general(a, b, (((1,), (0,)), ((), ())), preferred_element_type=F32)


def nt(a, b):
    return lax.dot_general(a, b, (((1,), (1,)), ((), ())), preferred_element_type=F32)


COPIES = 120
ORDER = (0, 3, 1, 2)
FORWARD = (
    (0, 0), (3, 0), (1, 0), (0, 3), (0, 1), (2, 0), (3, 3), (3, 1),
    (1, 3), (1, 1), (0, 2), (2, 3), (2, 1), (3, 2), (1, 2), (2, 2),
)
BACK_P = (2, 1, 3, 0)
BACKWARD = (
    (0, 2), (1, 2), (0, 1), (0, 3), (2, 2), (1, 1), (1, 3), (0, 0),
    (3, 2), (2, 1), (2, 3), (1, 0), (3, 1), (3, 3), (2, 0), (3, 0),
)


def layer_kernel(
    group,
    length_ref,
    limit_ref,
    ak_ref,
    av_ref,
    pk_ref,
    pv_ref,
    q_ref,
    g_ref,
    att_final,
    dq_final,
    ak_final,
    av_final,
    pk_final,
    pv_final,
    held,
    total,
    staged_ans,
    staged_pre,
    answers_in,
    prefix_in,
    native,
    split,
    rows_ref,
    weights,
    tops,
    top_now,
    row_sum,
    acc_t,
    douts,
    douts_t,
    delta_ref,
    masked_queries,
    probs_low,
    fin,
    ans_out,
    pre_out,
    far2,
    near2,
    far1,
    near1,
    ans_swap,
    pre_swap,
    pre_got,
    send_sem,
    recv_sem,
    local_sem,
):
    d = HEAD_DIM
    z, y, core = place()
    pos = q_ref.shape[1]
    batch = q_ref.shape[2]
    ans_rows = batch * pos
    pre_rows = pk_ref.shape[0]
    sources_total = RING * RING * CORES
    here_rows = CORES * pos
    rows = group * here_rows
    scale = d**-0.5
    factor = scale * LOG2E
    chip = z * RING + y
    pair = lax.axis_index("pair")
    block_rows, parts, mine, other = spans(ans_rows, pre_rows)
    pieces = (pl.ds(0, ans_rows), pl.ds(ans_rows, 2 * pre_rows))
    copies = Copies(send_sem, recv_sem)
    sources = (core, 1 - core)

    def held_at(r, dp, dq):
        zz, yy = shifted(sources[r], dp, dq)
        return held.at[zz, yy, sources[r]]

    def total_at(r, dp, dq):
        zz, yy = shifted(sources[r], dp, dq)
        return total.at[zz, yy, sources[r]]

    greet()
    small_fetches = [
        pltpu.make_async_copy(ref, small, local_sem.at[6 + n])
        for n, (ref, small) in enumerate(
            zip((ak_ref, av_ref, pk_ref, pv_ref), (answers_in.at[0], answers_in.at[1], prefix_in.at[0], prefix_in.at[1]))
        )
    ]

    def fetch(n):
        return pltpu.make_async_copy((q_ref, g_ref)[n].at[0], native.at[n], local_sem.at[n])

    for copy in small_fetches + [fetch(0), fetch(1)]:
        copy.start()
    for copy in small_fetches:
        copy.wait()
    for n in range(2):
        lanes = slice(n * d, (n + 1) * d)
        for c in range(CORES):
            head = slice(c * d, (c + 1) * d)
            staged_ans[c, :, lanes] = jnp.swapaxes(answers_in[n, 0, :, :, head], 0, 1).reshape(ans_rows, d)
            staged_pre[c, :, lanes] = prefix_in[n, :, head]
    met()
    loads = [
        pltpu.make_async_copy(staged_ans.at[core], held.at[z, y, core, pieces[0]], local_sem.at[2]),
        pltpu.make_async_copy(staged_pre.at[core], held.at[z, y, core, mine], local_sem.at[3]),
    ]
    for copy in loads:
        copy.start()
    there = held.at[z, y, core]
    copies.send(("sib", 0), lambda: (staged_ans.at[1 - core], there.at[pieces[0]], sibling()))
    copies.send(("sib", 1), lambda: (staged_pre.at[1 - core], there.at[mine], sibling()))
    copies.send(("pair", 0), lambda: (staged_pre.at[core], there.at[mine], across(True)))
    copies.send(("pair", 1), lambda: (staged_pre.at[1 - core], there.at[mine], across(False)))

    def own(r, piece):
        ref = held_at(r, 0, 0).at[pieces[piece]]
        source = staged_ans.at[core] if (r, piece) == (0, 0) else ref
        for direction in (1, 3):
            copies.send(
                ("one", r, direction, piece), lambda direction=direction: (source, ref, to(sources[r], direction, 0))
            )
        for direction in (1, 3):
            copies.send(
                ("two", r, 0, direction, piece), lambda direction=direction: (source, ref, to(sources[r], 0, direction))
            )

    def spread(k, piece):
        for r in range(2):
            for direction in (1, 3):

                def ends(r=r, direction=direction):
                    ref = held_at(r, ORDER[k], 0)
                    ref = ref if piece == 2 else ref.at[pieces[piece]]
                    return ref, ref, to(sources[r], 0, direction)

                copies.send(("two", r, k, direction, piece), ends)

    def head_lanes(c, g):
        return pl.ds(pl.multiple_of((c * group + g) * d, d), d)

    def lay_out(n):
        fetch(n).wait()
        for g in range(group):
            split[n, :, g] = jnp.swapaxes(native[n, :, :, head_lanes(1 - core, g)], 0, 1)
        copies.send(("q", n), lambda: (split.at[n], rows_ref.at[n, :, :, core], sibling()))
        for g in range(group):
            rows_ref[n, :, g, core] = jnp.swapaxes(native[n, :, :, head_lanes(core, g)], 0, 1)

    def laid_out(n):
        copies.arrived(("q", n), rows_ref.at[n, :, :, 1 - core], sibling())

    own(0, 0)
    lay_out(0)
    copies.arrived(("sib", 0), held_at(1, 0, 0).at[pieces[0]], sibling())
    own(1, 0)
    for copy in loads:
        copy.wait()
    copies.arrived(("pair", 0), held_at(0, 0, 0).at[other], across(True))
    own(0, 1)
    copies.arrived(("sib", 1), held_at(1, 0, 0).at[mine], sibling())
    copies.arrived(("pair", 1), held_at(1, 0, 0).at[other], across(False))
    own(1, 1)
    laid_out(0)

    def first_neighbours(piece):
        for direction in (1, 3):
            back = (-direction) % RING
            for r in range(2):
                copies.arrived(
                    ("one", r, direction, piece), held_at(r, back, 0).at[pieces[piece]], to(sources[r], direction, 0)
                )

                def ends(r=r, direction=direction, back=back):
                    ref = held_at(r, back, 0).at[parts[direction // 2]]
                    return ref, ref, to(sources[r], direction, 0)

                if piece == 1:
                    copies.send(("far", r, direction), ends)
            spread(ORDER.index(back), piece)

    def first_far():
        for r in range(2):
            for direction in (1, 3):
                copies.arrived(
                    ("far", r, direction), held_at(r, 2, 0).at[parts[direction // 2]], to(sources[r], direction, 0)
                )
        spread(3, 2)

    def second_neighbours(k):
        for direction in (1, 3):
            back = (-direction) % RING
            for r in range(2):
                here = held_at(r, ORDER[k], back)
                for piece in range(2) if k < 3 else (2,):
                    area = here if piece == 2 else here.at[pieces[piece]]
                    copies.arrived(("two", r, k, direction, piece), area, to(sources[r], 0, direction))

                def ends(r=r, direction=direction, back=back):
                    ref = held_at(r, ORDER[k], back).at[parts[direction // 2]]
                    return ref, ref, to(sources[r], 0, direction)

                copies.send(("far2", r, k, direction), ends)

    def second_far(k):
        for r in range(2):
            here = held_at(r, ORDER[k], 2)
            for direction in (1, 3):
                copies.arrived(("far2", r, k, direction), here.at[parts[direction // 2]], to(sources[r], 0, direction))

    forward_steps = {
        1: lambda: (first_neighbours(0), first_neighbours(1)),
        2: lambda: lay_out(1),
        3: lambda: second_neighbours(0),
        5: first_far,
        6: lambda: second_neighbours(1),
        8: lambda: second_neighbours(2),
        10: lambda: second_far(0),
        11: lambda: second_neighbours(3),
        13: lambda: second_far(1),
        14: lambda: second_far(2),
        15: lambda: second_far(3),
    }
    top_now[...] = jnp.full_like(top_now, NEGATIVE)
    row_sum[...] = jnp.zeros_like(row_sum)
    acc_t[...] = jnp.zeros_like(acc_t)

    def cat(b, dp, dq, lanes):
        spots = [held_at(r, dp, dq) for r in range(2)]
        return jnp.concatenate(
            [spot[b * pos : (b + 1) * pos, lanes] for spot in spots] + [spot[ans_rows:block_rows, lanes] for spot in spots],
            axis=0,
        )

    keys_at, values_at = slice(0, d), slice(d, 2 * d)

    def mask_features(b, dp, dq):
        limit = limit_ref[0, b]

        def one_hot(feature):
            lane = lax.broadcasted_iota(jnp.int32, feature.shape, 1)
            return jnp.where(lane == feature, 1.0, 0.0)

        ans_part, pre_part = [], []
        for r in range(2):
            zz, yy = shifted(sources[r], dp, dq)
            source = (zz * RING + yy) * CORES + sources[r]
            key = lax.broadcasted_iota(jnp.int32, (pos, d), 0) + (source * pos - chip * here_rows)
            ans_part.append(one_hot(jnp.where(key <= 0, -1, jnp.where(key < here_rows, key, 0))))
            for p in range(2):
                token = lax.broadcasted_iota(jnp.int32, (pre_rows, d), 0) + (p * sources_total + source) * pre_rows
                pre_part.append(one_hot(jnp.where(token < limit, -1, 0)))
        return jnp.concatenate(ans_part + pre_part, axis=0).astype(BF16)

    def query_rows(n, b):
        return rows_ref[n, b].reshape(rows, d)

    tiles = [slice(lo, min(lo + 2 * d, rows)) for lo in range(0, rows, 2 * d)]
    mask_row = lax.broadcasted_iota(jnp.int32, (here_rows, d), 0)
    mask_lane = lax.broadcasted_iota(jnp.int32, (here_rows, d), 1)
    row_mask = jnp.where((mask_lane == 0) | (mask_lane > mask_row), NEGATIVE, 0.0).astype(BF16)
    for b in range(batch):
        masked_queries[b, :, 0:d] = query_rows(0, b)
        for g in range(group):
            masked_queries[b, g * here_rows : (g + 1) * here_rows, d : 2 * d] = row_mask

    @pl.loop(0, RING * RING)
    def _(i):
        for n, step in forward_steps.items():
            run_at(i == n, step)
        dp = pick(i, [f[0] for f in FORWARD])
        dq = pick(i, [f[1] for f in FORWARD])
        at = dp * RING + dq
        def softmax(b, span, scores):
            before = top_now[b, :, span]
            folded = jnp.max(scores.reshape(-1, 8, scores.shape[1]), axis=0)
            now = jnp.maximum(before, jnp.max(folded, axis=0, keepdims=True))
            top_now[b, :, span] = now
            tops[b, at, :, span] = now
            ratio = jnp.exp2((before - now) * factor)
            e = jnp.exp2(scores * factor - now[0:1] * factor)
            row_sum[b, :, span] = row_sum[b, :, span] * ratio + jnp.sum(e.reshape(-1, 8, e.shape[1]), axis=0)
            low = e.astype(BF16)
            weights[b, at, :, span] = low
            return ratio, low

        keys = [
            jnp.concatenate([cat(b, dp, dq, keys_at), mask_features(b, dp, dq)], axis=1) for b in range(batch)
        ]
        values_t = [cat(b, dp, dq, values_at).T for b in range(batch)]

        scores = [[nt(keys[b], masked_queries[b, span]) for span in tiles] for b in range(batch)]
        for b in range(batch):
            ratios = []
            for span, tile in zip(tiles, scores[b]):
                ratios.append(softmax(b, span, tile)[0][0:1])
            acc_t[b] = acc_t[b] * jnp.concatenate(ratios, axis=1) + nn(values_t[b], weights[b, at])

    laid_out(1)
    for b in range(batch):
        inverse = 1.0 / jnp.sum(row_sum[b], axis=0, keepdims=True)
        attended_t = acc_t[b] * inverse
        alive = lax.broadcasted_iota(jnp.int32, (here_rows, d), 0) + chip * here_rows < length_ref[0, b]
        alive = jnp.concatenate([jnp.where(alive, 1.0, 0.0)] * group, axis=0)
        live_grad = jnp.where(alive > 0.5, query_rows(1, b).astype(F32), 0.0)
        scaled_t = (live_grad.T * inverse).astype(BF16)
        delta_ref[b] = jnp.broadcast_to(
            jnp.sum(scaled_t.astype(F32) * attended_t, axis=0, keepdims=True), delta_ref.shape[1:]
        )
        douts_t[b] = scaled_t
        douts[b] = scaled_t.astype(F32).T.astype(BF16)
        attended = jnp.where(alive > 0.5, attended_t.T, 0.0).astype(BF16)
        rows_ref[1, b] = attended.reshape(rows_ref.shape[2:])
        acc_t[b] = jnp.zeros_like(acc_t[b])

    rows_final = (att_final, dq_final)

    def leave(n):
        copies.send(("out", n), lambda: (rows_ref.at[1 - n, :, :, 1 - core], fin.at[n], sibling()))
        for g in range(group):
            rows_final[n][0, :, :, head_lanes(core, g)] = jnp.swapaxes(rows_ref[1 - n, :, g, core], 0, 1)

    def settle_rows(n):
        copies.arrived(("out", n), fin.at[n], sibling())
        for g in range(group):
            rows_final[n][0, :, :, head_lanes(1 - core, g)] = jnp.swapaxes(fin[n, :, g], 0, 1)

    leave(0)

    def add(into, other_ref):
        into[...] = (into[...].astype(F32) + other_ref[...].astype(F32)).astype(BF16)

    def far(k):
        for r in range(2):
            for n, direction in enumerate((1, 3)):

                def ends(r=r, n=n, direction=direction):
                    ref = total_at(r, BACK_P[k], 2).at[parts[n]]
                    return ref, far2.at[r, k, n], to(sources[r], 0, direction)

                copies.send(("back far2", r, k, n), ends)

    tail_pieces = (pieces[1], pieces[0])

    def near(k, piece=None):
        for r in range(2):
            for n, direction in enumerate((1, 3)):
                if piece != 1:
                    copies.arrived(("back far2", r, k, n), far2.at[r, k, n], to(sources[r], 0, direction))
                    add(total_at(r, BACK_P[k], direction).at[parts[n]], far2.at[r, k, n])

                def ends(r=r, n=n, direction=direction):
                    source, target = total_at(r, BACK_P[k], direction), near2.at[r, k, n]
                    if piece is not None:
                        source, target = source.at[tail_pieces[piece]], target.at[tail_pieces[piece]]
                    return source, target, to(sources[r], 0, direction)

                copies.send(("back near2", r, k, n, piece), ends)

    def settle(k):
        for r in range(2):
            for n, direction in enumerate((1, 3)):
                copies.arrived(("back near2", r, k, n, None), near2.at[r, k, n], to(sources[r], 0, direction))
            into = total_at(r, BACK_P[k], 0)
            into[...] = (
                into[...].astype(F32) + near2[r, k, 0].astype(F32) + near2[r, k, 1].astype(F32)
            ).astype(BF16)

    def far_first():
        for r in range(2):
            for n, direction in enumerate((1, 3)):

                def ends(r=r, n=n, direction=direction):
                    return total_at(r, 2, 0).at[parts[n]], far1.at[r, n], to(sources[r], direction, 0)

                copies.send(("back far1", r, n), ends)

    def near_first(k, piece):
        n, direction = k - 1, BACK_P[k]
        for r in range(2):
            if piece == 0:
                copies.arrived(("back far1", r, n), far1.at[r, n], to(sources[r], direction, 0))
                add(total_at(r, direction, 0).at[parts[n]], far1.at[r, n])

            def ends(r=r):
                area = tail_pieces[piece]
                return total_at(r, direction, 0).at[area], near1.at[r, n, area], to(sources[r], direction, 0)

            copies.send(("back near1", r, n, piece), ends)

    def finish_piece(piece):
        for r in range(2):
            for n, direction in enumerate((1, 3)):
                area = tail_pieces[piece]
                copies.arrived(("back near2", r, 3, n, piece), near2.at[r, 3, n, area], to(sources[r], 0, direction))
                copies.arrived(("back near1", r, n, piece), near1.at[r, n, area], to(sources[r], direction, 0))

    def final(r, area):
        parts_in = (near2[r, 3, 0, area], near2[r, 3, 1, area], near1[r, 0, area], near1[r, 1, area])
        value = total_at(r, 0, 0)[area].astype(F32)
        for part in parts_in:
            value = value + part.astype(F32)
        return value

    back_steps = {
        0: lambda: far(0),
        1: lambda: (far(1), settle_rows(0)),
        3: lambda: near(0),
        4: lambda: far(2),
        6: lambda: near(1),
        8: lambda: (far(3), settle(0), far_first()),
        10: lambda: near(2),
        11: lambda: (settle(1), near_first(1, 0)),
        13: lambda: near(3, 0),
        14: lambda: (settle(2), near_first(2, 0), near(3, 1), near_first(1, 1), near_first(2, 1)),
    }

    @pl.loop(0, RING * RING)
    def _(j):
        dp = pick(j, [BACK_P[f[0]] for f in BACKWARD])
        dq = pick(j, [f[1] for f in BACKWARD])
        at = dp * RING + dq
        key_terms, value_terms = [], []
        for b in range(batch):
            values = cat(b, dp, dq, values_at)
            for span in tiles:
                ratio = jnp.exp2((tops[b, at, :, span] - top_now[b, :, span]) * factor)[0:1]
                low = (weights[b, at, :, span].astype(F32) * ratio).astype(BF16)
                probs_low[b, :, span] = low
                grad_probs = nn(values, douts_t[b, :, span])
                grad_low = low.astype(F32) * (grad_probs - delta_ref[b, 0:1, span])
                weights[b, at, :, span] = grad_low.astype(BF16)
            value_terms.append(nn(probs_low[b], douts[b]))
            key_terms.append(nn(weights[b, at], query_rows(0, b)) * scale)
        for lanes, terms in ((keys_at, key_terms), (values_at, value_terms)):
            prefix = sum(terms)[CORES * pos :]
            for r in range(2):
                spot = total_at(r, dp, dq)
                for b in range(batch):
                    spot[b * pos : (b + 1) * pos, lanes] = terms[b][r * pos : (r + 1) * pos].astype(BF16)
                spot[ans_rows:block_rows, lanes] = prefix[r * 2 * pre_rows : (r + 1) * 2 * pre_rows].astype(BF16)
        for n, step in back_steps.items():
            run_at(j == n, step)

    finish_piece(0)
    for r in (1, 0):
        pre_swap[r, 0] = final(r, other).astype(BF16)
        if r == 1:
            copies.send(("pre", 1, 0), lambda: (pre_swap.at[1, 0], pre_got.at[1, 0], across(False)))
            pre_swap[1, 1] = final(1, mine).astype(BF16)
            copies.send(("pre", 1, 1), lambda: (pre_swap.at[1, 1], pre_got.at[1, 1], sibling()))
        else:
            copies.send(("pre", 0, 0), lambda: (pre_swap.at[0, 0], pre_got.at[0, 0], across(True)))
            pre_out[core] = final(0, mine)

    @pl.loop(0, RING)
    def _(dp):
        for b in range(batch):
            keys = jnp.concatenate([cat(b, dp, dq, keys_at).T for dq in range(RING)], axis=1)
            grads = weights[b, pl.ds(dp * RING, RING)]
            acc_t[b] += nn(keys, grads.reshape(-1, rows))

    for b in range(batch):
        rows_ref[0, b] = (acc_t[b] * scale).T.astype(BF16).reshape(rows_ref.shape[2:])
    leave(1)
    finish_piece(1)
    ans_swap[...] = final(1, pieces[0]).astype(BF16)
    copies.send(("ans",), lambda: (ans_swap, ans_out.at[core], sibling()))
    ans_out[core] = final(0, pieces[0]).astype(BF16)
    settle_rows(1)
    copies.arrived(("pre", 1, 1), pre_got.at[1, 1], sibling())
    copies.arrived(("pre", 1, 0), pre_got.at[1, 0], across(False))
    pre_out[1 - core] = pre_got[1, 0].astype(F32) + pre_got[1, 1].astype(F32)
    copies.arrived(("pre", 0, 0), pre_got.at[0, 0], across(True))
    pre_out[core] = pre_out[core] + pre_got[0, 0].astype(F32)
    copies.arrived(("ans",), ans_out.at[1 - core], sibling())
    for n, (answer, prefix) in enumerate(((ak_final, pk_final), (av_final, pv_final))):
        lanes = slice(n * d, (n + 1) * d)
        for c in range(CORES):
            head = slice(c * d, (c + 1) * d)
            prefix[:, head] = pre_out[c, :, lanes]
            answer[0, :, :, head] = jnp.swapaxes(ans_out[c, :, lanes].reshape(-1, pos, d), 0, 1)
    copies.finish()


def layer(lengths, limits, answer_keys, answer_values, prefix_keys, prefix_values, queries, grad_out):
    d = HEAD_DIM
    _, pos, batch, features = queries.shape
    group = features // d // CORES
    rows, width = group * CORES * pos, 2 * d
    ans_rows, pre_rows = batch * pos, prefix_keys.shape[0]
    block = ans_rows + 2 * pre_rows
    half = block // 2
    groups = RING * RING
    keys = CORES * (pos + 2 * pre_rows)
    vmem = pl.BlockSpec(memory_space=pltpu.VMEM)
    smem = pl.BlockSpec(memory_space=pltpu.SMEM)
    anywhere = pl.BlockSpec(memory_space=pl.ANY)
    tokens = pltpu.VMEM(queries.shape, BF16)
    answers = pltpu.VMEM(answer_keys.shape, BF16)
    prefix = pltpu.VMEM(prefix_keys.shape, F32)
    per_head = (batch, group, pos, d)
    return pl.pallas_call(
        functools.partial(layer_kernel, group),
        out_shape=(tokens, tokens, answers, answers, prefix, prefix),
        in_specs=[smem] * 2 + [anywhere] * 6,
        out_specs=(vmem,) * 6,
        scratch_shapes=[
            pltpu.VMEM((RING, RING, CORES, block, width), BF16),
            pltpu.VMEM((RING, RING, CORES, block, width), BF16),
            pltpu.VMEM((CORES, ans_rows, width), BF16),
            pltpu.VMEM((CORES, pre_rows, width), BF16),
            pltpu.VMEM((2,) + answer_keys.shape, BF16),
            pltpu.VMEM((2,) + prefix_keys.shape, BF16),
            pltpu.VMEM((2, pos, batch, features), BF16),
            pltpu.VMEM((2,) + per_head, BF16),
            pltpu.VMEM((2, batch, group, CORES, pos, d), BF16),
            pltpu.VMEM((batch, groups, keys, rows), BF16),
            pltpu.VMEM((batch, groups, 8, rows), F32),
            pltpu.VMEM((batch, 8, rows), F32),
            pltpu.VMEM((batch, 8, rows), F32),
            pltpu.VMEM((batch, d, rows), F32),
            pltpu.VMEM((batch, rows, d), BF16),
            pltpu.VMEM((batch, d, rows), BF16),
            pltpu.VMEM((batch, 8, rows), F32),
            pltpu.VMEM((batch, rows, 2 * d), BF16),
            pltpu.VMEM((batch, keys, rows), BF16),
            pltpu.VMEM((2,) + per_head, BF16),
            pltpu.VMEM((CORES, ans_rows, width), BF16),
            pltpu.VMEM((CORES, pre_rows, width), F32),
            pltpu.VMEM((CORES, RING, 2, half, width), BF16),
            pltpu.VMEM((CORES, RING, 2, block, width), BF16),
            pltpu.VMEM((CORES, 2, half, width), BF16),
            pltpu.VMEM((CORES, 2, block, width), BF16),
            pltpu.VMEM((ans_rows, width), BF16),
            pltpu.VMEM((2, 2, pre_rows, width), BF16),
            pltpu.VMEM((2, 2, pre_rows, width), BF16),
            pltpu.SemaphoreType.DMA((COPIES,)),
            pltpu.SemaphoreType.DMA((COPIES,)),
            pltpu.SemaphoreType.DMA((10,)),
        ],
        compiler_params=pltpu.CompilerParams(
            collective_id=0, has_side_effects=True, vmem_limit_bytes=58 * 1024 * 1024
        ),
        name="layer",
    )(lengths, limits, answer_keys, answer_values, prefix_keys, prefix_values, queries, grad_out)


def settle_kernel(count, *refs):
    ins, outs, sems = refs[:count], refs[count : 2 * count], refs[2 * count]
    gives = [pltpu.make_async_copy(ins[n], outs[n], sems.at[n]) for n in range(count)]
    for copy in gives:
        copy.start()
    for copy in gives:
        copy.wait()


def settle_results(results):
    count = len(results)
    return pl.pallas_call(
        functools.partial(settle_kernel, count),
        out_shape=tuple(jax.ShapeDtypeStruct(x.shape, x.dtype) for x in results),
        in_specs=[pl.BlockSpec(memory_space=pltpu.VMEM)] * count,
        out_specs=(pl.BlockSpec(memory_space=pl.ANY),) * count,
        scratch_shapes=[pltpu.SemaphoreType.DMA((count,))],
        name="settle",
    )(*[pltpu.with_memory_space_constraint(x, pltpu.VMEM) for x in results])


def on_device(
    queries,
    answer_keys,
    answer_values,
    prefix_keys,
    prefix_values,
    grad_out,
    answer_length,
    prefix_limit,
):
    return settle_results(
        layer(
            answer_length,
            prefix_limit,
            answer_keys,
            answer_values,
            prefix_keys,
            prefix_values,
            queries,
            grad_out,
        )
    )


def solution(mesh):
    tokens = P("pair", "seq", None, "head")
    prefix = P(("pair", "seq"), "head")
    scalars = P("pair", None)
    return jax.shard_map(
        on_device,
        mesh=mesh,
        in_specs=(tokens, tokens, tokens, prefix, prefix, tokens, scalars, scalars),
        out_specs=(tokens, tokens, tokens, tokens, prefix, prefix),
        check_vma=False,
    )
```

```python
import functools

import jax
import jax.numpy as jnp
from jax import lax
from jax.experimental import pallas as pl
from jax.experimental.pallas import tpu as pltpu
from jax.sharding import PartitionSpec as P

HEAD_DIM = 128
RING = 4
CORES = 2
LOG2E = 1.4426950408889634
NEGATIVE = -1e30
MESH = pl.DeviceIdType.MESH
BF16 = jnp.bfloat16
F32 = jnp.float32


def place():
    s = lax.axis_index("seq")
    return s // (RING * CORES), (s // CORES) % RING, s % CORES


def seq_of(z, y, core):
    return (z * RING + y) * CORES + core


def shifted(h, dp, dq):
    z, y, _ = place()
    return (z + dp * h + dq * (1 - h)) % RING, (y + dp * (1 - h) + dq * h) % RING


def to(h, dp, dq):
    z, y = shifted(h, dp, dq)
    return {"seq": seq_of(z, y, place()[2])}


def across(same_core):
    z, y, core = place()
    target = {"pair": 1 - lax.axis_index("pair")}
    if not same_core:
        target["seq"] = seq_of(z, y, 1 - core)
    return target


def sibling():
    z, y, core = place()
    return {"seq": seq_of(z, y, 1 - core)}


PEERS = 7


def greet():
    barrier = pltpu.get_barrier_semaphore()
    peers = [to(h, d, 0) for h in range(2) for d in (1, RING - 1)]
    peers += [sibling(), across(True), across(False)]
    for peer in peers:
        pl.semaphore_signal(barrier, inc=1, device_id=peer, device_id_type=MESH)


def met():
    pl.semaphore_wait(pltpu.get_barrier_semaphore(), PEERS)


def spans(ans_rows, pre_rows):
    pair = lax.axis_index("pair")
    rows = ans_rows + 2 * pre_rows
    half = rows // 2
    parts = (pl.ds(0, half), pl.ds(half, rows - half))
    mine = pl.ds(pl.multiple_of(ans_rows + pair * pre_rows, 16), pre_rows)
    other = pl.ds(pl.multiple_of(ans_rows + (1 - pair) * pre_rows, 16), pre_rows)
    return rows, parts, mine, other


class Copies:
    def __init__(self, send_sem, recv_sem):
        self.send_sem, self.recv_sem = send_sem, recv_sem
        self.ids = {}
        self.sent = []

    def make(self, key, src, dst, to):
        n = self.ids.setdefault(key, len(self.ids))
        return pltpu.make_async_remote_copy(
            src_ref=src,
            dst_ref=dst,
            send_sem=self.send_sem.at[n],
            recv_sem=self.recv_sem.at[n],
            device_id=to,
            device_id_type=MESH,
        )

    def send(self, key, ends):
        self.make(key, *ends()).start()
        self.sent.append((key, ends))

    def arrived(self, key, dst, to):
        self.make(key, dst, dst, to).wait_recv()

    def finish(self):
        for key, ends in self.sent:
            self.make(key, *ends()).wait_send()


def pick(i, values):
    chosen = jnp.int32(values[0])
    for n in range(1, len(values)):
        chosen = jnp.where(i == n, jnp.int32(values[n]), chosen)
    return chosen


def run_at(condition, step):
    @pl.when(condition)
    def _():
        step()


def nn(a, b):
    return lax.dot_general(a, b, (((1,), (0,)), ((), ())), preferred_element_type=F32)


def nt(a, b):
    return lax.dot_general(a, b, (((1,), (1,)), ((), ())), preferred_element_type=F32)


COPIES = 120
ORDER = (0, 3, 1, 2)
FORWARD = (
    (0, 0), (3, 0), (1, 0), (0, 3), (0, 1), (2, 0), (3, 3), (3, 1),
    (1, 3), (1, 1), (0, 2), (2, 3), (2, 1), (3, 2), (1, 2), (2, 2),
)
BACK_P = (2, 1, 3, 0)
BACKWARD = (
    (0, 2), (1, 2), (0, 1), (0, 3), (2, 2), (1, 1), (1, 3), (0, 0),
    (3, 2), (2, 1), (2, 3), (1, 0), (3, 1), (3, 3), (2, 0), (3, 0),
)


def layer_kernel(
    group,
    length_ref,
    limit_ref,
    ak_ref,
    av_ref,
    pk_ref,
    pv_ref,
    q_ref,
    g_ref,
    att_final,
    dq_final,
    ak_final,
    av_final,
    pk_final,
    pv_final,
    held,
    total,
    staged_ans,
    staged_pre,
    answers_in,
    prefix_in,
    native,
    split,
    rows_ref,
    weights,
    tops,
    top_now,
    row_sum,
    acc_t,
    douts,
    douts_t,
    delta_ref,
    masked_queries,
    probs_low,
    fin,
    ans_out,
    pre_out,
    far2,
    near2,
    far1,
    near1,
    ans_swap,
    pre_swap,
    pre_got,
    send_sem,
    recv_sem,
    local_sem,
):
    d = HEAD_DIM
    z, y, core = place()
    pos = q_ref.shape[1]
    batch = q_ref.shape[2]
    ans_rows = batch * pos
    pre_rows = pk_ref.shape[0]
    sources_total = RING * RING * CORES
    here_rows = CORES * pos
    rows = group * here_rows
    scale = d**-0.5
    factor = scale * LOG2E
    chip = z * RING + y
    pair = lax.axis_index("pair")
    block_rows, parts, mine, other = spans(ans_rows, pre_rows)
    pieces = (pl.ds(0, ans_rows), pl.ds(ans_rows, 2 * pre_rows))
    copies = Copies(send_sem, recv_sem)
    sources = (core, 1 - core)

    def held_at(r, dp, dq):
        zz, yy = shifted(sources[r], dp, dq)
        return held.at[zz, yy, sources[r]]

    def total_at(r, dp, dq):
        zz, yy = shifted(sources[r], dp, dq)
        return total.at[zz, yy, sources[r]]

    greet()
    small_fetches = [
        pltpu.make_async_copy(ref, small, local_sem.at[6 + n])
        for n, (ref, small) in enumerate(
            zip((ak_ref, av_ref, pk_ref, pv_ref), (answers_in.at[0], answers_in.at[1], prefix_in.at[0], prefix_in.at[1]))
        )
    ]

    def fetch(n):
        return pltpu.make_async_copy((q_ref, g_ref)[n].at[0], native.at[n], local_sem.at[n])

    for copy in small_fetches + [fetch(0), fetch(1)]:
        copy.start()
    for copy in small_fetches:
        copy.wait()
    for n in range(2):
        lanes = slice(n * d, (n + 1) * d)
        for c in range(CORES):
            head = slice(c * d, (c + 1) * d)
            staged_ans[c, :, lanes] = jnp.swapaxes(answers_in[n, 0, :, :, head], 0, 1).reshape(ans_rows, d)
            staged_pre[c, :, lanes] = prefix_in[n, :, head]
    met()
    loads = [
        pltpu.make_async_copy(staged_ans.at[core], held.at[z, y, core, pieces[0]], local_sem.at[2]),
        pltpu.make_async_copy(staged_pre.at[core], held.at[z, y, core, mine], local_sem.at[3]),
    ]
    for copy in loads:
        copy.start()
    there = held.at[z, y, core]
    copies.send(("sib", 0), lambda: (staged_ans.at[1 - core], there.at[pieces[0]], sibling()))
    copies.send(("sib", 1), lambda: (staged_pre.at[1 - core], there.at[mine], sibling()))
    copies.send(("pair", 0), lambda: (staged_pre.at[core], there.at[mine], across(True)))
    copies.send(("pair", 1), lambda: (staged_pre.at[1 - core], there.at[mine], across(False)))

    def own(r, piece, axis):
        ref = held_at(r, 0, 0).at[pieces[piece]]
        source = staged_ans.at[core] if (r, piece) == (0, 0) else ref
        for direction in (1, 3):
            key = ("one", r, direction, piece) if axis == 0 else ("two", r, 0, direction, piece)
            step = (direction, 0) if axis == 0 else (0, direction)
            copies.send(key, lambda step=step: (source, ref, to(sources[r], *step)))

    def spread(k, piece):
        for r in range(2):
            for direction in (1, 3):

                def ends(r=r, direction=direction):
                    ref = held_at(r, ORDER[k], 0)
                    ref = ref if piece == 2 else ref.at[pieces[piece]]
                    return ref, ref, to(sources[r], 0, direction)

                copies.send(("two", r, k, direction, piece), ends)

    def head_lanes(c, g):
        return pl.ds(pl.multiple_of((c * group + g) * d, d), d)

    def lay_out(n):
        fetch(n).wait()
        for g in range(group):
            split[n, :, g] = jnp.swapaxes(native[n, :, :, head_lanes(1 - core, g)], 0, 1)
        copies.send(("q", n), lambda: (split.at[n], rows_ref.at[n, :, :, core], sibling()))
        for g in range(group):
            rows_ref[n, :, g, core] = jnp.swapaxes(native[n, :, :, head_lanes(core, g)], 0, 1)

    def laid_out(n):
        copies.arrived(("q", n), rows_ref.at[n, :, :, 1 - core], sibling())

    own(0, 0, 0)
    own(0, 0, 1)
    lay_out(0)
    copies.arrived(("sib", 0), held_at(1, 0, 0).at[pieces[0]], sibling())
    own(1, 0, 0)
    own(1, 0, 1)
    for copy in loads:
        copy.wait()
    copies.arrived(("pair", 0), held_at(0, 0, 0).at[other], across(True))
    own(0, 1, 0)
    copies.arrived(("sib", 1), held_at(1, 0, 0).at[mine], sibling())
    copies.arrived(("pair", 1), held_at(1, 0, 0).at[other], across(False))
    own(1, 1, 0)
    own(0, 1, 1)
    own(1, 1, 1)
    laid_out(0)

    def first_neighbours(piece):
        for direction in (1, 3):
            back = (-direction) % RING
            for r in range(2):
                copies.arrived(
                    ("one", r, direction, piece), held_at(r, back, 0).at[pieces[piece]], to(sources[r], direction, 0)
                )

                def ends(r=r, direction=direction, back=back):
                    ref = held_at(r, back, 0).at[parts[direction // 2]]
                    return ref, ref, to(sources[r], direction, 0)

                if piece == 1:
                    copies.send(("far", r, direction), ends)
            spread(ORDER.index(back), piece)

    def first_far():
        for r in range(2):
            for direction in (1, 3):
                copies.arrived(
                    ("far", r, direction), held_at(r, 2, 0).at[parts[direction // 2]], to(sources[r], direction, 0)
                )
        spread(3, 2)

    def second_neighbours(k):
        for direction in (1, 3):
            back = (-direction) % RING
            for r in range(2):
                here = held_at(r, ORDER[k], back)
                for piece in range(2) if k < 3 else (2,):
                    area = here if piece == 2 else here.at[pieces[piece]]
                    copies.arrived(("two", r, k, direction, piece), area, to(sources[r], 0, direction))

                def ends(r=r, direction=direction, back=back):
                    ref = held_at(r, ORDER[k], back).at[parts[direction // 2]]
                    return ref, ref, to(sources[r], 0, direction)

                copies.send(("far2", r, k, direction), ends)

    def second_far(k):
        for r in range(2):
            here = held_at(r, ORDER[k], 2)
            for direction in (1, 3):
                copies.arrived(("far2", r, k, direction), here.at[parts[direction // 2]], to(sources[r], 0, direction))

    forward_steps = {
        1: lambda: (first_neighbours(0), lay_out(1), first_neighbours(1)),
        3: lambda: second_neighbours(0),
        5: first_far,
        6: lambda: second_neighbours(1),
        8: lambda: second_neighbours(2),
        10: lambda: second_far(0),
        11: lambda: second_neighbours(3),
        13: lambda: second_far(1),
        14: lambda: second_far(2),
        15: lambda: second_far(3),
    }
    top_now[...] = jnp.full_like(top_now, NEGATIVE)
    row_sum[...] = jnp.zeros_like(row_sum)
    acc_t[...] = jnp.zeros_like(acc_t)

    def cat(b, dp, dq, lanes):
        spots = [held_at(r, dp, dq) for r in range(2)]
        return jnp.concatenate(
            [spot[b * pos : (b + 1) * pos, lanes] for spot in spots] + [spot[ans_rows:block_rows, lanes] for spot in spots],
            axis=0,
        )

    keys_at, values_at = slice(0, d), slice(d, 2 * d)

    def mask_features(b, dp, dq):
        limit = limit_ref[0, b]

        def one_hot(feature):
            lane = lax.broadcasted_iota(jnp.int32, feature.shape, 1)
            return jnp.where(lane == feature, 1.0, 0.0)

        ans_part, pre_part = [], []
        for r in range(2):
            zz, yy = shifted(sources[r], dp, dq)
            source = (zz * RING + yy) * CORES + sources[r]
            key = lax.broadcasted_iota(jnp.int32, (pos, d), 0) + (source * pos - chip * here_rows)
            ans_part.append(one_hot(jnp.where(key <= 0, -1, jnp.where(key < here_rows, key, 0))))
            for p in range(2):
                token = lax.broadcasted_iota(jnp.int32, (pre_rows, d), 0) + (p * sources_total + source) * pre_rows
                pre_part.append(one_hot(jnp.where(token < limit, -1, 0)))
        return jnp.concatenate(ans_part + pre_part, axis=0).astype(BF16)

    def query_rows(n, b):
        return rows_ref[n, b].reshape(rows, d)

    tiles = [slice(lo, min(lo + 2 * d, rows)) for lo in range(0, rows, 2 * d)]
    mask_row = lax.broadcasted_iota(jnp.int32, (here_rows, d), 0)
    mask_lane = lax.broadcasted_iota(jnp.int32, (here_rows, d), 1)
    row_mask = jnp.where((mask_lane == 0) | (mask_lane > mask_row), NEGATIVE, 0.0).astype(BF16)
    for b in range(batch):
        masked_queries[b, :, 0:d] = query_rows(0, b)
        for g in range(group):
            masked_queries[b, g * here_rows : (g + 1) * here_rows, d : 2 * d] = row_mask

    @pl.loop(0, RING * RING)
    def _(i):
        for n, step in forward_steps.items():
            run_at(i == n, step)
        dp = pick(i, [f[0] for f in FORWARD])
        dq = pick(i, [f[1] for f in FORWARD])
        at = dp * RING + dq
        def softmax(b, span, scores):
            before = top_now[b, :, span]
            folded = jnp.max(scores.reshape(-1, 8, scores.shape[1]), axis=0)
            now = jnp.maximum(before, jnp.max(folded, axis=0, keepdims=True))
            top_now[b, :, span] = now
            tops[b, at, :, span] = now
            ratio = jnp.exp2((before - now) * factor)
            e = jnp.exp2(scores * factor - now[0:1] * factor)
            row_sum[b, :, span] = row_sum[b, :, span] * ratio + jnp.sum(e.reshape(-1, 8, e.shape[1]), axis=0)
            low = e.astype(BF16)
            weights[b, at, :, span] = low
            return ratio, low

        keys = [
            jnp.concatenate([cat(b, dp, dq, keys_at), mask_features(b, dp, dq)], axis=1) for b in range(batch)
        ]
        values_t = [cat(b, dp, dq, values_at).T for b in range(batch)]

        scores = [[nt(keys[b], masked_queries[b, span]) for span in tiles] for b in range(batch)]
        for b in range(batch):
            ratios = []
            for span, tile in zip(tiles, scores[b]):
                ratios.append(softmax(b, span, tile)[0][0:1])
            acc_t[b] = acc_t[b] * jnp.concatenate(ratios, axis=1) + nn(values_t[b], weights[b, at])

    laid_out(1)
    for b in range(batch):
        inverse = 1.0 / jnp.sum(row_sum[b], axis=0, keepdims=True)
        attended_t = acc_t[b] * inverse
        alive = lax.broadcasted_iota(jnp.int32, (here_rows, d), 0) + chip * here_rows < length_ref[0, b]
        alive = jnp.concatenate([jnp.where(alive, 1.0, 0.0)] * group, axis=0)
        live_grad = jnp.where(alive > 0.5, query_rows(1, b).astype(F32), 0.0)
        scaled_t = (live_grad.T * inverse).astype(BF16)
        delta_ref[b] = jnp.broadcast_to(
            jnp.sum(scaled_t.astype(F32) * attended_t, axis=0, keepdims=True), delta_ref.shape[1:]
        )
        douts_t[b] = scaled_t
        douts[b] = scaled_t.astype(F32).T.astype(BF16)
        attended = jnp.where(alive > 0.5, attended_t.T, 0.0).astype(BF16)
        rows_ref[1, b] = attended.reshape(rows_ref.shape[2:])
        acc_t[b] = jnp.zeros_like(acc_t[b])

    rows_final = (att_final, dq_final)

    def leave(n):
        copies.send(("out", n), lambda: (rows_ref.at[1 - n, :, :, 1 - core], fin.at[n], sibling()))
        for g in range(group):
            rows_final[n][0, :, :, head_lanes(core, g)] = jnp.swapaxes(rows_ref[1 - n, :, g, core], 0, 1)

    def settle_rows(n):
        copies.arrived(("out", n), fin.at[n], sibling())
        for g in range(group):
            rows_final[n][0, :, :, head_lanes(1 - core, g)] = jnp.swapaxes(fin[n, :, g], 0, 1)

    leave(0)

    def add(into, other_ref):
        into[...] = (into[...].astype(F32) + other_ref[...].astype(F32)).astype(BF16)

    def far(k):
        for r in range(2):
            for n, direction in enumerate((1, 3)):

                def ends(r=r, n=n, direction=direction):
                    ref = total_at(r, BACK_P[k], 2).at[parts[n]]
                    return ref, far2.at[r, k, n], to(sources[r], 0, direction)

                copies.send(("back far2", r, k, n), ends)

    tail_pieces = (pieces[1], pieces[0])

    def near(k, piece=None):
        for r in range(2):
            for n, direction in enumerate((1, 3)):
                if piece != 1:
                    copies.arrived(("back far2", r, k, n), far2.at[r, k, n], to(sources[r], 0, direction))
                    add(total_at(r, BACK_P[k], direction).at[parts[n]], far2.at[r, k, n])

                def ends(r=r, n=n, direction=direction):
                    source, target = total_at(r, BACK_P[k], direction), near2.at[r, k, n]
                    if piece is not None:
                        source, target = source.at[tail_pieces[piece]], target.at[tail_pieces[piece]]
                    return source, target, to(sources[r], 0, direction)

                copies.send(("back near2", r, k, n, piece), ends)

    def settle(k):
        for r in range(2):
            for n, direction in enumerate((1, 3)):
                copies.arrived(("back near2", r, k, n, None), near2.at[r, k, n], to(sources[r], 0, direction))
            into = total_at(r, BACK_P[k], 0)
            into[...] = (
                into[...].astype(F32) + near2[r, k, 0].astype(F32) + near2[r, k, 1].astype(F32)
            ).astype(BF16)

    def far_first():
        for r in range(2):
            for n, direction in enumerate((1, 3)):

                def ends(r=r, n=n, direction=direction):
                    return total_at(r, 2, 0).at[parts[n]], far1.at[r, n], to(sources[r], direction, 0)

                copies.send(("back far1", r, n), ends)

    def near_first(k, piece):
        n, direction = k - 1, BACK_P[k]
        for r in range(2):
            if piece == 0:
                copies.arrived(("back far1", r, n), far1.at[r, n], to(sources[r], direction, 0))
                add(total_at(r, direction, 0).at[parts[n]], far1.at[r, n])

            def ends(r=r):
                area = tail_pieces[piece]
                return total_at(r, direction, 0).at[area], near1.at[r, n, area], to(sources[r], direction, 0)

            copies.send(("back near1", r, n, piece), ends)

    def finish_piece(piece):
        for r in range(2):
            for n, direction in enumerate((1, 3)):
                area = tail_pieces[piece]
                copies.arrived(("back near2", r, 3, n, piece), near2.at[r, 3, n, area], to(sources[r], 0, direction))
                copies.arrived(("back near1", r, n, piece), near1.at[r, n, area], to(sources[r], direction, 0))

    def final(r, area):
        parts_in = (near2[r, 3, 0, area], near2[r, 3, 1, area], near1[r, 0, area], near1[r, 1, area])
        value = total_at(r, 0, 0)[area].astype(F32)
        for part in parts_in:
            value = value + part.astype(F32)
        return value

    back_steps = {
        0: lambda: far(0),
        1: lambda: (far(1), settle_rows(0)),
        3: lambda: near(0),
        4: lambda: far(2),
        6: lambda: near(1),
        8: lambda: (far(3), settle(0), far_first()),
        10: lambda: near(2),
        11: lambda: (settle(1), near_first(1, 0)),
        13: lambda: near(3, 0),
        14: lambda: (settle(2), near_first(2, 0), near(3, 1), near_first(1, 1), near_first(2, 1)),
    }

    @pl.loop(0, RING * RING)
    def _(j):
        dp = pick(j, [BACK_P[f[0]] for f in BACKWARD])
        dq = pick(j, [f[1] for f in BACKWARD])
        at = dp * RING + dq
        key_terms, value_terms = [], []
        for b in range(batch):
            values = cat(b, dp, dq, values_at)
            for span in tiles:
                ratio = jnp.exp2((tops[b, at, :, span] - top_now[b, :, span]) * factor)[0:1]
                low = (weights[b, at, :, span].astype(F32) * ratio).astype(BF16)
                probs_low[b, :, span] = low
                grad_probs = nn(values, douts_t[b, :, span])
                grad_low = low.astype(F32) * (grad_probs - delta_ref[b, 0:1, span])
                weights[b, at, :, span] = grad_low.astype(BF16)
            value_terms.append(nn(probs_low[b], douts[b]))
            key_terms.append(nn(weights[b, at], query_rows(0, b)) * scale)
        for lanes, terms in ((keys_at, key_terms), (values_at, value_terms)):
            prefix = sum(terms)[CORES * pos :]
            for r in range(2):
                spot = total_at(r, dp, dq)
                for b in range(batch):
                    spot[b * pos : (b + 1) * pos, lanes] = terms[b][r * pos : (r + 1) * pos].astype(BF16)
                spot[ans_rows:block_rows, lanes] = prefix[r * 2 * pre_rows : (r + 1) * 2 * pre_rows].astype(BF16)
        for n, step in back_steps.items():
            run_at(j == n, step)

    finish_piece(0)
    for r in (1, 0):
        pre_swap[r, 0] = final(r, other).astype(BF16)
        if r == 1:
            copies.send(("pre", 1, 0), lambda: (pre_swap.at[1, 0], pre_got.at[1, 0], across(False)))
            pre_swap[1, 1] = final(1, mine).astype(BF16)
            copies.send(("pre", 1, 1), lambda: (pre_swap.at[1, 1], pre_got.at[1, 1], sibling()))
        else:
            copies.send(("pre", 0, 0), lambda: (pre_swap.at[0, 0], pre_got.at[0, 0], across(True)))
            pre_out[core] = final(0, mine)

    @pl.loop(0, RING)
    def _(dp):
        for b in range(batch):
            keys = jnp.concatenate([cat(b, dp, dq, keys_at).T for dq in range(RING)], axis=1)
            grads = weights[b, pl.ds(dp * RING, RING)]
            acc_t[b] += nn(keys, grads.reshape(-1, rows))

    for b in range(batch):
        rows_ref[0, b] = (acc_t[b] * scale).T.astype(BF16).reshape(rows_ref.shape[2:])
    leave(1)
    finish_piece(1)
    ans_swap[...] = final(1, pieces[0]).astype(BF16)
    copies.send(("ans",), lambda: (ans_swap, ans_out.at[core], sibling()))
    ans_out[core] = final(0, pieces[0]).astype(BF16)
    settle_rows(1)
    copies.arrived(("pre", 1, 1), pre_got.at[1, 1], sibling())
    copies.arrived(("pre", 1, 0), pre_got.at[1, 0], across(False))
    pre_out[1 - core] = pre_got[1, 0].astype(F32) + pre_got[1, 1].astype(F32)
    copies.arrived(("pre", 0, 0), pre_got.at[0, 0], across(True))
    pre_out[core] = pre_out[core] + pre_got[0, 0].astype(F32)
    copies.arrived(("ans",), ans_out.at[1 - core], sibling())
    for n, (answer, prefix) in enumerate(((ak_final, pk_final), (av_final, pv_final))):
        lanes = slice(n * d, (n + 1) * d)
        for c in range(CORES):
            head = slice(c * d, (c + 1) * d)
            prefix[:, head] = pre_out[c, :, lanes]
            answer[0, :, :, head] = jnp.swapaxes(ans_out[c, :, lanes].reshape(-1, pos, d), 0, 1)
    copies.finish()


def layer(lengths, limits, answer_keys, answer_values, prefix_keys, prefix_values, queries, grad_out):
    d = HEAD_DIM
    _, pos, batch, features = queries.shape
    group = features // d // CORES
    rows, width = group * CORES * pos, 2 * d
    ans_rows, pre_rows = batch * pos, prefix_keys.shape[0]
    block = ans_rows + 2 * pre_rows
    half = block // 2
    groups = RING * RING
    keys = CORES * (pos + 2 * pre_rows)
    vmem = pl.BlockSpec(memory_space=pltpu.VMEM)
    smem = pl.BlockSpec(memory_space=pltpu.SMEM)
    anywhere = pl.BlockSpec(memory_space=pl.ANY)
    tokens = pltpu.VMEM(queries.shape, BF16)
    answers = pltpu.VMEM(answer_keys.shape, BF16)
    prefix = pltpu.VMEM(prefix_keys.shape, F32)
    per_head = (batch, group, pos, d)
    return pl.pallas_call(
        functools.partial(layer_kernel, group),
        out_shape=(tokens, tokens, answers, answers, prefix, prefix),
        in_specs=[smem] * 2 + [anywhere] * 6,
        out_specs=(vmem,) * 6,
        scratch_shapes=[
            pltpu.VMEM((RING, RING, CORES, block, width), BF16),
            pltpu.VMEM((RING, RING, CORES, block, width), BF16),
            pltpu.VMEM((CORES, ans_rows, width), BF16),
            pltpu.VMEM((CORES, pre_rows, width), BF16),
            pltpu.VMEM((2,) + answer_keys.shape, BF16),
            pltpu.VMEM((2,) + prefix_keys.shape, BF16),
            pltpu.VMEM((2, pos, batch, features), BF16),
            pltpu.VMEM((2,) + per_head, BF16),
            pltpu.VMEM((2, batch, group, CORES, pos, d), BF16),
            pltpu.VMEM((batch, groups, keys, rows), BF16),
            pltpu.VMEM((batch, groups, 8, rows), F32),
            pltpu.VMEM((batch, 8, rows), F32),
            pltpu.VMEM((batch, 8, rows), F32),
            pltpu.VMEM((batch, d, rows), F32),
            pltpu.VMEM((batch, rows, d), BF16),
            pltpu.VMEM((batch, d, rows), BF16),
            pltpu.VMEM((batch, 8, rows), F32),
            pltpu.VMEM((batch, rows, 2 * d), BF16),
            pltpu.VMEM((batch, keys, rows), BF16),
            pltpu.VMEM((2,) + per_head, BF16),
            pltpu.VMEM((CORES, ans_rows, width), BF16),
            pltpu.VMEM((CORES, pre_rows, width), F32),
            pltpu.VMEM((CORES, RING, 2, half, width), BF16),
            pltpu.VMEM((CORES, RING, 2, block, width), BF16),
            pltpu.VMEM((CORES, 2, half, width), BF16),
            pltpu.VMEM((CORES, 2, block, width), BF16),
            pltpu.VMEM((ans_rows, width), BF16),
            pltpu.VMEM((2, 2, pre_rows, width), BF16),
            pltpu.VMEM((2, 2, pre_rows, width), BF16),
            pltpu.SemaphoreType.DMA((COPIES,)),
            pltpu.SemaphoreType.DMA((COPIES,)),
            pltpu.SemaphoreType.DMA((10,)),
        ],
        compiler_params=pltpu.CompilerParams(
            collective_id=0, has_side_effects=True, vmem_limit_bytes=58 * 1024 * 1024
        ),
        name="layer",
    )(lengths, limits, answer_keys, answer_values, prefix_keys, prefix_values, queries, grad_out)


def settle_kernel(count, *refs):
    ins, outs, sems = refs[:count], refs[count : 2 * count], refs[2 * count]
    gives = [pltpu.make_async_copy(ins[n], outs[n], sems.at[n]) for n in range(count)]
    for copy in gives:
        copy.start()
    for copy in gives:
        copy.wait()


def settle_results(results):
    count = len(results)
    return pl.pallas_call(
        functools.partial(settle_kernel, count),
        out_shape=tuple(jax.ShapeDtypeStruct(x.shape, x.dtype) for x in results),
        in_specs=[pl.BlockSpec(memory_space=pltpu.VMEM)] * count,
        out_specs=(pl.BlockSpec(memory_space=pl.ANY),) * count,
        scratch_shapes=[pltpu.SemaphoreType.DMA((count,))],
        name="settle",
    )(*[pltpu.with_memory_space_constraint(x, pltpu.VMEM) for x in results])


def on_device(
    queries,
    answer_keys,
    answer_values,
    prefix_keys,
    prefix_values,
    grad_out,
    answer_length,
    prefix_limit,
):
    return settle_results(
        layer(
            answer_length,
            prefix_limit,
            answer_keys,
            answer_values,
            prefix_keys,
            prefix_values,
            queries,
            grad_out,
        )
    )


def solution(mesh):
    tokens = P("pair", "seq", None, "head")
    prefix = P(("pair", "seq"), "head")
    scalars = P("pair", None)
    return jax.shard_map(
        on_device,
        mesh=mesh,
        in_specs=(tokens, tokens, tokens, prefix, prefix, tokens, scalars, scalars),
        out_specs=(tokens, tokens, tokens, tokens, prefix, prefix),
        check_vma=False,
    )
```
